32 devices in a mesh: dp: 1 (over z), tp: 32 (over y, x, core).
Axes of the slice: x: 4, y: 4, z: 1, core: 2. Of those that a mesh axis runs over, the one named last changes fastest.
The devices are a block of a 4x4x8 slice.
Arguments:
- x_in: bfloat16 [2048, 4096], P('dp')
- g_norm: bfloat16 [4096], replicated
- w_q: bfloat16 [4096, 4096], P(None, 'tp')
- w_k: bfloat16 [4096, 1024], replicated
- w_v: bfloat16 [4096, 1024], replicated
- w_o: bfloat16 [4096, 4096], P('tp')
- w_gate: bfloat16 [4096, 14336], P(None, 'tp')
- w_up: bfloat16 [4096, 14336], P(None, 'tp')
- w_down: bfloat16 [14336, 4096], P('tp')
Outputs:
- output 1: bfloat16 [2048, 4096], P('dp')
- output 2: bfloat16 [2048, 32, 128], P('dp', 'tp')
- output 3: bfloat16 [2048, 32, 128], P('dp', 'tp')
All inputs are finite; a program needn't handle non-finite values.
Results may differ from the reference program's by a relative error of at most 0.0147537.
Values are sent between devices in bfloat16 or wider.
A program may use at most 768 MiB of HBM per device.

```python
import math
import jax
import jax.numpy as jnp
from jax import lax

TOKENS = 2048
D = 4096
HEADS = 32
KV_HEADS = 8
HEAD = 128
FF = 14336
KV_SLOTS = 32
QBLOCK = 128

ROPE_BASE = 500000.0
NORM_EPS = 1e-5


def setup_inputs(seed: int = 0, part: int = 0) -> dict:
    key_list = jax.random.split(jax.random.key(seed), 10)
    part_key = jax.random.fold_in(key_list[9], part)
    q_gain = math.sqrt(math.log(TOKENS / 16.0)) / 1.09
    x_val = 0.7 * jax.random.normal(part_key, (TOKENS, D), jnp.float32)
    g_val = jnp.exp(0.7 * jax.random.normal(key_list[0], (D,), jnp.float32) - 0.49)
    w_q = jax.random.normal(key_list[1], (D, HEADS * HEAD), jnp.float32) * (q_gain / math.sqrt(D))
    w_k = jax.random.normal(key_list[2], (D, KV_HEADS * HEAD), jnp.float32) / math.sqrt(D)
    w_v = jax.random.normal(key_list[3], (D, KV_HEADS * HEAD), jnp.float32) / math.sqrt(D)
    w_o = jax.random.normal(key_list[4], (HEADS * HEAD, D), jnp.float32) * (3.0 / math.sqrt(HEADS * HEAD))
    w_gate = jax.random.normal(key_list[5], (D, FF), jnp.float32) / math.sqrt(D)
    w_up = jax.random.normal(key_list[6], (D, FF), jnp.float32) / math.sqrt(D)
    w_down = jax.random.normal(key_list[7], (FF, D), jnp.float32) / math.sqrt(FF)
    return {'x_in': x_val.astype(jnp.bfloat16), 'g_norm': g_val.astype(jnp.bfloat16), 'w_q': w_q.astype(jnp.bfloat16), 'w_k': w_k.astype(jnp.bfloat16), 'w_v': w_v.astype(jnp.bfloat16), 'w_o': w_o.astype(jnp.bfloat16), 'w_gate': w_gate.astype(jnp.bfloat16), 'w_up': w_up.astype(jnp.bfloat16), 'w_down': w_down.astype(jnp.bfloat16)}


def rope_tables(positions):
    inv_freq = ROPE_BASE ** (-jnp.arange(0, HEAD, 2, dtype=jnp.float32) / HEAD)
    angles = positions.astype(jnp.float32)[:, None] * inv_freq[None, :]
    return jnp.cos(angles), jnp.sin(angles)


def apply_rope(projected, cos_tab, sin_tab):
    half_dim = HEAD // 2
    lower_half = projected[..., :half_dim]
    upper_half = projected[..., half_dim:]
    cos_b = cos_tab[:, None, :]
    sin_b = sin_tab[:, None, :]
    return jnp.concatenate([lower_half * cos_b - upper_half * sin_b, upper_half * cos_b + lower_half * sin_b], axis=-1)


def reference(x_in, g_norm, w_q, w_k, w_v, w_o, w_gate, w_up, w_down):
    x_f32 = x_in.astype(jnp.float32)
    inv_rms = lax.rsqrt(jnp.mean(x_f32 * x_f32, axis=-1, keepdims=True) + NORM_EPS)
    normed = (x_f32 * inv_rms * g_norm.astype(jnp.float32)).astype(jnp.bfloat16)
    cos_tab, sin_tab = rope_tables(jnp.arange(TOKENS))
    q_proj = jnp.dot(normed, w_q, preferred_element_type=jnp.float32).reshape(TOKENS, HEADS, HEAD)
    k_proj = jnp.dot(normed, w_k, preferred_element_type=jnp.float32).reshape(TOKENS, KV_HEADS, HEAD)
    q_rot = apply_rope(q_proj, cos_tab, sin_tab).astype(jnp.bfloat16)
    k_rot = apply_rope(k_proj, cos_tab, sin_tab).astype(jnp.bfloat16)
    v_proj = jnp.dot(normed, w_v, preferred_element_type=jnp.float32).astype(jnp.bfloat16).reshape(TOKENS, KV_HEADS, HEAD)
    group_size = HEADS // KV_HEADS
    q_grouped = q_rot.reshape(TOKENS, KV_HEADS, group_size, HEAD)
    k_f32 = k_rot.astype(jnp.float32)
    v_f32 = v_proj.astype(jnp.float32)
    score_scale = 1.0 / math.sqrt(HEAD)
    key_pos = jnp.arange(TOKENS)

    def attend_block(block_idx):
        row_start = block_idx * QBLOCK
        q_part = lax.dynamic_slice_in_dim(q_grouped, row_start, QBLOCK, axis=0).astype(jnp.float32)
        scores = jnp.einsum('qgrd,kgd->grqk', q_part, k_f32) * score_scale
        query_pos = row_start + jnp.arange(QBLOCK)
        visible = key_pos[None, :] <= query_pos[:, None]
        scores = jnp.where(visible, scores, -1e30)
        probs = jax.nn.softmax(scores, axis=-1).astype(jnp.bfloat16).astype(jnp.float32)
        return jnp.einsum('grqk,kgd->qgrd', probs, v_f32).astype(jnp.bfloat16)

    attn_blocks = lax.map(attend_block, jnp.arange(TOKENS // QBLOCK))
    attn_out = attn_blocks.reshape(TOKENS, HEADS * HEAD)
    attn_sum = jnp.dot(attn_out, w_o, preferred_element_type=jnp.float32)
    gate_proj = jnp.dot(normed, w_gate, preferred_element_type=jnp.float32)
    up_proj = jnp.dot(normed, w_up, preferred_element_type=jnp.float32)
    hidden = (jax.nn.silu(gate_proj) * up_proj).astype(jnp.bfloat16)
    mlp_sum = jnp.dot(hidden, w_down, preferred_element_type=jnp.float32)
    y_out = (x_f32 + attn_sum + mlp_sum).astype(jnp.bfloat16)
    slot_repeat = KV_SLOTS // KV_HEADS
    k_cache = jnp.repeat(k_rot, slot_repeat, axis=1)
    v_cache = jnp.repeat(v_proj, slot_repeat, axis=1)
    return (y_out, k_cache, v_cache)
```

```python
import functools
import math
import jax
import jax.numpy as jnp
from jax import lax
from jax.experimental import pallas as pl
from jax.experimental.pallas import tpu as pltpu
from jax.sharding import PartitionSpec as P

HEAD_DIM = 128
ROPE_BASE = 500000.0
NORM_EPS = 1e-5
LANES = 128
ROWS = 128
KEYS = 512
OUT_TILE = 1024
LAG = (0, 1, 2, 3, 4, 5, 6, 7, 8, 9, 10)
BF16 = jnp.bfloat16
F32 = jnp.float32


def layer_kernel(cfg, x_hbm, g_ref, cos_hbm, sin_hbm, wq_hbm, wk_hbm, wv_hbm, wo_hbm, wg_hbm, wu_hbm, wd_hbm,
                 y_hbm, k_hbm, v_hbm,
                 wqkv, wg, wu, wod, xbuf, tabs, abuf, ombuf, kbuf, vbuf, part, quart, r1, r2, r3, r4, xres, ybuf,
                 wsem, xsem, ressem, kvsem, ysem, pair_send, pair_recv, ssem, rsem, gpair_send, gpair_recv):
    tokens, width = x_hbm.shape
    tp, side, kv_heads = cfg
    nblk = tokens // ROWS
    half = width // 2
    quarter = half // 2
    cw = quarter // side
    ch = cw // 2
    rw = ROWS // side
    ff = wg.shape[1]

    me = lax.axis_index("tp")
    core = lax.rem(me, 2)
    px = lax.rem(me // 2, side)
    py = me // (2 * side)
    partner = me + 1 - 2 * core

    def wrap(p):
        return lax.rem(p + side, side)

    def at(y, x):
        return (wrap(y) * side + wrap(x)) * 2 + core

    near = (((at(py, px + 1)), (at(py, px - 1))), ((at(py + 1, px)), (at(py - 1, px))))
    pos = (px, py)

    def dev(d):
        return {"tp": d}

    barrier = pltpu.get_barrier_semaphore()
    for d in (partner, *near[0], *near[1]):
        pl.semaphore_signal(barrier, inc=1, device_id=dev(d), device_id_type=pl.DeviceIdType.MESH)

    head = lax.div(me * kv_heads, tp)
    kcol = pl.ds(pl.multiple_of(head * HEAD_DIM, HEAD_DIM), HEAD_DIM)
    mine0 = core * half
    res_col = [pl.multiple_of(mine0 + ab * quarter + pos[ab] * cw, cw) for ab in (0, 1)]

    def x_load(b, slot):
        rows = pl.ds(pl.multiple_of(b * ROWS, ROWS), ROWS)
        return (pltpu.make_async_copy(x_hbm.at[rows], xbuf.at[slot], xsem.at[slot, 0]),
                pltpu.make_async_copy(cos_hbm.at[rows], tabs.at[slot, 0], xsem.at[slot, 1]),
                pltpu.make_async_copy(sin_hbm.at[rows], tabs.at[slot, 1], xsem.at[slot, 2]))

    w_loads = (
        pltpu.make_async_copy(wq_hbm, wqkv.at[:, pl.ds(0, HEAD_DIM)], wsem.at[0]),
        pltpu.make_async_copy(wk_hbm.at[:, kcol], wqkv.at[:, pl.ds(HEAD_DIM, HEAD_DIM)], wsem.at[1]),
        pltpu.make_async_copy(wv_hbm.at[:, kcol], wqkv.at[:, pl.ds(2 * HEAD_DIM, HEAD_DIM)], wsem.at[2]),
        pltpu.make_async_copy(wg_hbm, wg, wsem.at[3]),
        pltpu.make_async_copy(wu_hbm, wu, wsem.at[4]),
        pltpu.make_async_copy(wo_hbm, wod.at[pl.ds(0, HEAD_DIM)], wsem.at[5]),
        pltpu.make_async_copy(wd_hbm, wod.at[pl.ds(HEAD_DIM, ff)], wsem.at[6]),
    )
    for c in x_load(0, 0):
        c.start()
    for c in w_loads:
        c.start()
    res_loads = [pltpu.make_async_copy(x_hbm.at[:, pl.ds(res_col[ab], cw)], xres.at[ab], ressem.at[ab]) for ab in (0, 1)]
    for c in res_loads:
        c.start()
    kbuf[...] = jnp.zeros_like(kbuf)
    vbuf[...] = jnp.zeros_like(vbuf)

    def pair_copy(b):
        col = pl.multiple_of((1 - core) * half, half)
        return pltpu.make_async_remote_copy(
            src_ref=part.at[lax.rem(b, 2), :, pl.ds(col, half)], dst_ref=quart.at[b],
            send_sem=pair_send.at[lax.rem(b, 2)], recv_sem=pair_recv.at[b],
            device_id=dev(partner), device_id_type=pl.DeviceIdType.MESH)

    def hop(src, dst, st, b, ab, d, axis):
        return pltpu.make_async_remote_copy(
            src_ref=src, dst_ref=dst, send_sem=ssem.at[st, ab, d, lax.rem(b, 2)], recv_sem=rsem.at[st, ab, d, b],
            device_id=dev(near[axis][d]), device_id_type=pl.DeviceIdType.MESH)

    def qcols(ab, chunk, h=None):
        base = ab * quarter + wrap(chunk) * cw
        if h is None:
            return pl.ds(pl.multiple_of(base, cw), cw)
        return pl.ds(pl.multiple_of(base + h * ch, ch), ch)

    def ycols(ab, chunk, h=None):
        base = mine0 + ab * quarter + wrap(chunk) * cw
        if h is None:
            return pl.ds(pl.multiple_of(base, cw), cw)
        return pl.ds(pl.multiple_of(base + h * ch, ch), ch)

    def brows(chunk):
        return pl.ds(pl.multiple_of(wrap(chunk) * rw, rw), rw)

    def yrows(b, chunk=None):
        if chunk is None:
            return pl.ds(pl.multiple_of(b * ROWS, ROWS), ROWS)
        return pl.ds(pl.multiple_of(b * ROWS + wrap(chunk) * rw, rw), rw)

    def send1(b, ab, d):
        p = pos[ab]
        return hop(quart.at[b, :, qcols(ab, p + 2, d)], r1.at[b, ab, d], 0, b, ab, d, ab)

    def send2(b, ab, d):
        p = pos[ab]
        return hop(quart.at[b, :, qcols(ab, p + 1 - 2 * d)], r2.at[b, ab, d], 1, b, ab, d, ab)

    def send3(b, ab, d):
        p2 = pos[1 - ab]
        return hop(quart.at[b, brows(p2 + 2), qcols(ab, pos[ab], d)], r3.at[b, ab, d], 2, b, ab, d, 1 - ab)

    def send4(b, ab, d):
        p2 = pos[1 - ab]
        return hop(quart.at[b, brows(p2 + 1 - 2 * d), qcols(ab, pos[ab])], r4.at[b, ab, d], 3, b, ab, d, 1 - ab)

    def y_hop(b, rows, cols, st, ab, d, axis):
        return hop(ybuf.at[rows, cols], ybuf.at[rows, cols], st, b, ab, d, axis)

    def send5(b, ab, d):
        return y_hop(b, yrows(b, pos[1 - ab]), ycols(ab, pos[ab]), 4, ab, d, 1 - ab)

    def land5(b, ab, d):
        return y_hop(b, yrows(b, pos[1 - ab] - 1 + 2 * d), ycols(ab, pos[ab]), 4, ab, d, 1 - ab)

    def send6(b, ab, d):
        return y_hop(b, yrows(b, pos[1 - ab] - 1 + 2 * d), ycols(ab, pos[ab], d), 5, ab, d, 1 - ab)

    def land6(b, ab, d):
        return y_hop(b, yrows(b, pos[1 - ab] + 2), ycols(ab, pos[ab], d), 5, ab, d, 1 - ab)

    def send7(b, ab, d):
        return y_hop(b, yrows(b), ycols(ab, pos[ab]), 6, ab, d, ab)

    def land7(b, ab, d):
        return y_hop(b, yrows(b), ycols(ab, pos[ab] - 1 + 2 * d), 6, ab, d, ab)

    def send8(b, ab, d):
        return y_hop(b, yrows(b), ycols(ab, pos[ab] - 1 + 2 * d, d), 7, ab, d, ab)

    def land8(b, ab, d):
        return y_hop(b, yrows(b), ycols(ab, pos[ab] + 2, d), 7, ab, d, ab)

    sends = (send1, send2, send3, send4, send5, send6, send7, send8)

    def gpair(b, c):
        cols = pl.ds(pl.multiple_of(c * half, half), half)
        return pltpu.make_async_remote_copy(
            src_ref=ybuf.at[yrows(b), cols], dst_ref=ybuf.at[yrows(b), cols],
            send_sem=gpair_send.at[lax.rem(b, 2)], recv_sem=gpair_recv.at[b],
            device_id=dev(partner), device_id_type=pl.DeviceIdType.MESH)

    def y_store(b):
        return pltpu.make_async_copy(ybuf.at[yrows(b)], y_hbm.at[yrows(b)], ysem.at[lax.rem(b, 2)])

    def kv_store(b):
        rows = yrows(b)
        slot = lax.rem(b, 2)
        return (pltpu.make_async_copy(kbuf.at[rows], k_hbm.at[rows], kvsem.at[slot, 0]),
                pltpu.make_async_copy(vbuf.at[rows], v_hbm.at[rows], kvsem.at[slot, 1]))

    def issue(send, b):
        for ab in (0, 1):
            for d in (0, 1):
                @pl.when(b >= 2)
                def _():
                    send(b - 2, ab, d).wait_send()
                send(b, ab, d).start()

    def attend(q, b, keys):
        ks = kbuf[pl.ds(0, keys), :]
        s = lax.dot_general(q, ks, (((1,), (1,)), ((), ())), preferred_element_type=F32)
        s = s * (1.0 / math.sqrt(HEAD_DIM))
        qpos = b * ROWS + lax.broadcasted_iota(jnp.int32, s.shape, 0)
        kpos = lax.broadcasted_iota(jnp.int32, s.shape, 1)
        s = jnp.where(kpos <= qpos, s, -1e30)
        top = jnp.max(s, axis=-1, keepdims=True)
        e = jnp.exp(s - top)
        probs = (e * (1.0 / jnp.sum(e, axis=-1, keepdims=True))).astype(BF16)
        o = jnp.dot(probs, vbuf[pl.ds(0, keys), :], preferred_element_type=F32)
        ombuf[:, pl.ds(0, HEAD_DIM)] = o.astype(BF16)

    def compute(b):
        slot = lax.rem(b, 2)
        for c in x_load(b, slot):
            c.wait()

        @pl.when(b + 1 < nblk)
        def _():
            for c in x_load(b + 1, 1 - slot):
                c.start()

        @pl.when(b == 0)
        def _():
            for c in w_loads[:3]:
                c.wait()

        for r in range(0, ROWS, 16):
            xr = xbuf[slot, pl.ds(r, 16), :].astype(F32)
            inv = lax.rsqrt(jnp.mean(xr * xr, axis=-1, keepdims=True) + NORM_EPS)
            abuf[pl.ds(r, 16), :] = (xr * inv * g_ref[...].astype(F32)).astype(BF16)

        a = abuf[...]
        qkv = jnp.dot(a, wqkv[...], preferred_element_type=F32)
        cos_t = tabs[slot, 0]
        sin_t = tabs[slot, 1]

        def rope(z):
            return (z * cos_t + pltpu.roll(z, HEAD_DIM // 2, 1) * sin_t).astype(BF16)

        q = rope(qkv[:, :HEAD_DIM])
        rows = yrows(b)
        kbuf[rows, :] = rope(qkv[:, HEAD_DIM:2 * HEAD_DIM])
        vbuf[rows, :] = qkv[:, 2 * HEAD_DIM:].astype(BF16)

        @pl.when(b >= 2)
        def _():
            for c in kv_store(b - 2):
                c.wait()

        for c in kv_store(b):
            c.start()

        for n in range(tokens // KEYS):
            @pl.when(b * ROWS // KEYS == n)
            def _(n=n):
                attend(q, b, (n + 1) * KEYS)

        @pl.when(b == 0)
        def _():
            for c in w_loads[3:]:
                c.wait()

        gate = jnp.dot(a, wg[...], preferred_element_type=F32)
        up = jnp.dot(a, wu[...], preferred_element_type=F32)
        ombuf[:, pl.ds(HEAD_DIM, ff)] = (gate * jax.nn.sigmoid(gate) * up).astype(BF16)

        @pl.when(b >= 2)
        def _():
            pair_copy(b - 2).wait_send()

        om = ombuf[...]
        for c0 in range(0, width, OUT_TILE):
            cols = pl.ds(c0, OUT_TILE)
            part[slot, :, cols] = jnp.dot(om, wod[:, cols], preferred_element_type=F32).astype(BF16)
        pair_copy(b).start()

    def add(dst, *srcs):
        total = dst[...].astype(F32)
        for s in srcs:
            total = total + s[...].astype(F32)
        dst[...] = total.astype(BF16)

    def both(f):
        for ab in (0, 1):
            for d in (0, 1):
                f(ab, d)

    def stage1(b):
        pair_copy(b).wait_recv()
        mine = pl.ds(pl.multiple_of(mine0, half), half)
        for r in range(0, ROWS, 32):
            add(quart.at[b, pl.ds(r, 32), :], part.at[lax.rem(b, 2), pl.ds(r, 32), mine])
        issue(send1, b)

    def stage2(b):
        both(lambda ab, d: send1(b, ab, d).wait_recv())
        both(lambda ab, d: add(quart.at[b, :, qcols(ab, pos[ab] + 1 - 2 * d, d)], r1.at[b, ab, d]))
        issue(send2, b)

    def stage3(b):
        both(lambda ab, d: send2(b, ab, d).wait_recv())
        for ab in (0, 1):
            add(quart.at[b, :, qcols(ab, pos[ab])], r2.at[b, ab, 0], r2.at[b, ab, 1])
        issue(send3, b)

    def stage4(b):
        both(lambda ab, d: send3(b, ab, d).wait_recv())
        both(lambda ab, d: add(quart.at[b, brows(pos[1 - ab] + 1 - 2 * d), qcols(ab, pos[ab], d)], r3.at[b, ab, d]))
        issue(send4, b)

    def stage5(b):
        @pl.when(b == 0)
        def _():
            for c in res_loads:
                c.wait()

        both(lambda ab, d: send4(b, ab, d).wait_recv())
        for ab in (0, 1):
            p2 = pos[1 - ab]
            total = quart[b, brows(p2), qcols(ab, pos[ab])].astype(F32)
            total = total + r4[b, ab, 0].astype(F32) + r4[b, ab, 1].astype(F32)
            total = total + xres[ab, yrows(b, p2), :].astype(F32)
            ybuf[yrows(b, p2), ycols(ab, pos[ab])] = total.astype(BF16)
        issue(send5, b)

    def stage6(b):
        both(lambda ab, d: land5(b, ab, d).wait_recv())
        issue(send6, b)

    def stage7(b):
        both(lambda ab, d: land6(b, ab, d).wait_recv())
        issue(send7, b)

    def stage8(b):
        both(lambda ab, d: land7(b, ab, d).wait_recv())
        issue(send8, b)

    def stage9(b):
        both(lambda ab, d: land8(b, ab, d).wait_recv())

        @pl.when(b >= 2)
        def _():
            gpair(b - 2, core).wait_send()

        gpair(b, core).start()

    def stage10(b):
        gpair(b, 1 - core).wait_recv()

        @pl.when(b >= 2)
        def _():
            y_store(b - 2).wait()

        y_store(b).start()

    stages = (compute, stage1, stage2, stage3, stage4, stage5, stage6, stage7, stage8, stage9, stage10)

    pl.semaphore_wait(barrier, 5)

    @pl.loop(0, nblk + LAG[-1])
    def _(t):
        for lag, stage in zip(LAG, stages):
            b = t - lag

            @pl.when((b >= 0) & (b < nblk))
            def _(b=b, stage=stage):
                stage(b)

    for b in range(nblk - 2, nblk):
        pair_copy(b).wait_send()
        for send in sends:
            both(lambda ab, d: send(b, ab, d).wait_send())
        gpair(b, core).wait_send()
        y_store(b).wait()
        for c in kv_store(b):
            c.wait()


def solution(mesh):
    tp_size = mesh.shape['tp']
    side = math.isqrt(tp_size // 2)

    def local_layer(x_in, g_norm, w_q, w_k, w_v, w_o, w_gate, w_up, w_down):
        tokens, width = x_in.shape
        kv_heads = w_k.shape[1] // HEAD_DIM
        ff = w_gate.shape[1]
        nblk = tokens // ROWS
        half = width // 2
        cw = half // 2 // side
        rw = ROWS // side
        inv_freq = ROPE_BASE ** (-jnp.arange(0, HEAD_DIM, 2, dtype=F32) / HEAD_DIM)
        angles = jnp.arange(tokens).astype(F32)[:, None] * inv_freq[None, :]
        cos_half, sin_half = jnp.cos(angles), jnp.sin(angles)
        cos_tab = jnp.concatenate([cos_half, cos_half], axis=1)
        sin_tab = jnp.concatenate([-sin_half, sin_half], axis=1)
        any_spec = pl.BlockSpec(memory_space=pl.ANY)
        y, k, v = pl.pallas_call(
            functools.partial(layer_kernel, (tp_size, side, kv_heads)),
            out_shape=(jax.ShapeDtypeStruct((tokens, width), BF16),
                       jax.ShapeDtypeStruct((tokens, HEAD_DIM), BF16),
                       jax.ShapeDtypeStruct((tokens, HEAD_DIM), BF16)),
            in_specs=[any_spec, pl.BlockSpec(memory_space=pltpu.VMEM)] + [any_spec] * 9,
            out_specs=(any_spec,) * 3,
            scratch_shapes=[
                pltpu.VMEM((width, 3 * HEAD_DIM), BF16),
                pltpu.VMEM((width, ff), BF16),
                pltpu.VMEM((width, ff), BF16),
                pltpu.VMEM((HEAD_DIM + ff, width), BF16),
                pltpu.VMEM((2, ROWS, width), BF16),
                pltpu.VMEM((2, 2, ROWS, HEAD_DIM), F32),
                pltpu.VMEM((ROWS, width), BF16),
                pltpu.VMEM((ROWS, HEAD_DIM + ff), BF16),
                pltpu.VMEM((tokens, HEAD_DIM), BF16),
                pltpu.VMEM((tokens, HEAD_DIM), BF16),
                pltpu.VMEM((2, ROWS, width), BF16),
                pltpu.VMEM((nblk, ROWS, half), BF16),
                pltpu.VMEM((nblk, 2, 2, ROWS, cw // 2), BF16),
                pltpu.VMEM((nblk, 2, 2, ROWS, cw), BF16),
                pltpu.VMEM((nblk, 2, 2, rw, cw // 2), BF16),
                pltpu.VMEM((nblk, 2, 2, rw, cw), BF16),
                pltpu.VMEM((2, tokens, cw), BF16),
                pltpu.VMEM((tokens, width), BF16),
                pltpu.SemaphoreType.DMA((7,)),
                pltpu.SemaphoreType.DMA((2, 3)),
                pltpu.SemaphoreType.DMA((2,)),
                pltpu.SemaphoreType.DMA((2, 2)),
                pltpu.SemaphoreType.DMA((2,)),
                pltpu.SemaphoreType.DMA((2,)),
                pltpu.SemaphoreType.DMA((nblk,)),
                pltpu.SemaphoreType.DMA((8, 2, 2, 2)),
                pltpu.SemaphoreType.DMA((8, 2, 2, nblk)),
                pltpu.SemaphoreType.DMA((2,)),
                pltpu.SemaphoreType.DMA((nblk,)),
            ],
            compiler_params=pltpu.CompilerParams(collective_id=0, has_side_effects=True, vmem_limit_bytes=67043328),
            name="layer",
        )(x_in, g_norm.reshape(1, width), cos_tab, sin_tab, w_q, w_k, w_v, w_o, w_gate, w_up, w_down)
        return y, k.reshape(tokens, 1, HEAD_DIM), v.reshape(tokens, 1, HEAD_DIM)

    return jax.shard_map(local_layer, mesh=mesh, in_specs=(P('dp', None), P(None), P(None, 'tp'), P(None, None), P(None, None), P('tp', None), P(None, 'tp'), P(None, 'tp'), P('tp', None)), out_specs=(P('dp', None), P('dp', 'tp', None), P('dp', 'tp', None)), check_vma=False)
```

```python
import functools
import math
import jax
import jax.numpy as jnp
import numpy as np
from jax import lax
from jax.experimental import pallas as pl
from jax.experimental.pallas import tpu as pltpu
from jax.sharding import PartitionSpec as P

HEAD_DIM = 128
ROPE_BASE = 500000.0
NORM_EPS = 1e-5
LANES = 128
ROWS = 128
PAIR = 2 * ROWS
SLOTS = 4
KEYS = 512
OUT_TILE = 1024
LAG = (2, 3, 4, 5, 6, 7, 8, 9, 10, 11)
BF16 = jnp.bfloat16
F32 = jnp.float32


def layer_kernel(cfg, x_hbm, g_ref, tab_hbm, wq_hbm, wk_hbm, wv_hbm, wo_hbm, wg_hbm, wu_hbm, wd_hbm,
                 ybuf, k_hbm, v_hbm,
                 wqkv, wgu, wod, xbuf, tabs, abuf, ombuf, kbuf, vbuf, part, quart, r1, r2, r3, r4, xres,
                 wsem, xsem, ressem, kvsem, pair_send, pair_recv, ssem, rsem, gpair_send, gpair_recv):
    tokens, width = x_hbm.shape
    tp, side, kv_heads = cfg
    nblk = tokens // ROWS
    half = width // 2
    quarter = half // 2
    cw = quarter // side
    ch = cw // 2
    rw = ROWS // side
    ff = wg_hbm.shape[0]

    me = lax.axis_index("tp")
    core = lax.rem(me, 2)
    px = lax.rem(me // 2, side)
    py = me // (2 * side)
    partner = me + 1 - 2 * core

    def wrap(p):
        return lax.rem(p + side, side)

    def at(y, x):
        return (wrap(y) * side + wrap(x)) * 2 + core

    near = (((at(py, px + 1)), (at(py, px - 1))), ((at(py + 1, px)), (at(py - 1, px))))
    pos = (px, py)

    def dev(d):
        return {"tp": d}

    barrier = pltpu.get_barrier_semaphore()
    for d in (partner, *near[0], *near[1]):
        pl.semaphore_signal(barrier, inc=1, device_id=dev(d), device_id_type=pl.DeviceIdType.MESH)

    head = lax.div(me * kv_heads, tp)
    kcol = pl.ds(pl.multiple_of(head * HEAD_DIM, HEAD_DIM), HEAD_DIM)
    mine0 = core * half
    res_col = [pl.multiple_of(mine0 + ab * quarter + pos[ab] * cw, cw) for ab in (0, 1)]

    def x_load(c, slot):
        rows = pl.ds(pl.multiple_of(c * PAIR, PAIR), PAIR)
        return (pltpu.make_async_copy(x_hbm.at[rows], xbuf.at[slot], xsem.at[slot, 0]),
                pltpu.make_async_copy(tab_hbm.at[:, rows], tabs.at[slot], xsem.at[slot, 1]))

    w_loads = (
        pltpu.make_async_copy(wq_hbm, wqkv.at[:, pl.ds(0, HEAD_DIM)], wsem.at[0]),
        pltpu.make_async_copy(wk_hbm.at[:, kcol], wqkv.at[:, pl.ds(HEAD_DIM, HEAD_DIM)], wsem.at[1]),
        pltpu.make_async_copy(wv_hbm.at[:, kcol], wqkv.at[:, pl.ds(2 * HEAD_DIM, HEAD_DIM)], wsem.at[2]),
        pltpu.make_async_copy(wg_hbm, wgu.at[pl.ds(0, ff)], wsem.at[3]),
        pltpu.make_async_copy(wu_hbm, wgu.at[pl.ds(ff, ff)], wsem.at[4]),
        pltpu.make_async_copy(wo_hbm, wod.at[pl.ds(0, HEAD_DIM)], wsem.at[5]),
        pltpu.make_async_copy(wd_hbm, wod.at[pl.ds(HEAD_DIM, ff)], wsem.at[6]),
    )
    for c in x_load(0, 0):
        c.start()
    for c in w_loads:
        c.start()
    res_loads = [pltpu.make_async_copy(x_hbm.at[:, pl.ds(res_col[ab], cw)], xres.at[ab], ressem.at[ab]) for ab in (0, 1)]
    for c in res_loads:
        c.start()
    kbuf[...] = jnp.zeros_like(kbuf)
    vbuf[...] = jnp.zeros_like(vbuf)

    def pair_copy(b):
        col = pl.multiple_of((1 - core) * half, half)
        return pltpu.make_async_remote_copy(
            src_ref=part.at[lax.rem(b, SLOTS), :, pl.ds(col, half)], dst_ref=quart.at[b],
            send_sem=pair_send.at[lax.rem(b, SLOTS)], recv_sem=pair_recv.at[b],
            device_id=dev(partner), device_id_type=pl.DeviceIdType.MESH)

    def hop(src, dst, st, b, ab, d, axis):
        return pltpu.make_async_remote_copy(
            src_ref=src, dst_ref=dst, send_sem=ssem.at[st, ab, d, lax.rem(b, 2)], recv_sem=rsem.at[st, ab, d, b],
            device_id=dev(near[axis][d]), device_id_type=pl.DeviceIdType.MESH)

    def qcols(ab, chunk, h=None):
        base = ab * quarter + wrap(chunk) * cw
        if h is None:
            return pl.ds(pl.multiple_of(base, cw), cw)
        return pl.ds(pl.multiple_of(base + h * ch, ch), ch)

    def ycols(ab, chunk, h=None):
        base = mine0 + ab * quarter + wrap(chunk) * cw
        if h is None:
            return pl.ds(pl.multiple_of(base, cw), cw)
        return pl.ds(pl.multiple_of(base + h * ch, ch), ch)

    def brows(chunk):
        return pl.ds(pl.multiple_of(wrap(chunk) * rw, rw), rw)

    def yrows(b, chunk=None):
        if chunk is None:
            return pl.ds(pl.multiple_of(b * ROWS, ROWS), ROWS)
        return pl.ds(pl.multiple_of(b * ROWS + wrap(chunk) * rw, rw), rw)

    def send1(b, ab, d):
        p = pos[ab]
        return hop(quart.at[b, :, qcols(ab, p + 2, d)], r1.at[lax.rem(b, SLOTS), ab, d], 0, b, ab, d, ab)

    def send2(b, ab, d):
        p = pos[ab]
        return hop(quart.at[b, :, qcols(ab, p + 1 - 2 * d)], r2.at[lax.rem(b, SLOTS), ab, d], 1, b, ab, d, ab)

    def send3(b, ab, d):
        p2 = pos[1 - ab]
        return hop(quart.at[b, brows(p2 + 2), qcols(ab, pos[ab], d)], r3.at[b, ab, d], 2, b, ab, d, 1 - ab)

    def send4(b, ab, d):
        p2 = pos[1 - ab]
        return hop(quart.at[b, brows(p2 + 1 - 2 * d), qcols(ab, pos[ab])], r4.at[b, ab, d], 3, b, ab, d, 1 - ab)

    def y_hop(b, rows, cols, st, ab, d, axis):
        return hop(ybuf.at[rows, cols], ybuf.at[rows, cols], st, b, ab, d, axis)

    def send5(b, ab, d):
        return y_hop(b, yrows(b, pos[1 - ab]), ycols(ab, pos[ab]), 4, ab, d, 1 - ab)

    def land5(b, ab, d):
        return y_hop(b, yrows(b, pos[1 - ab] - 1 + 2 * d), ycols(ab, pos[ab]), 4, ab, d, 1 - ab)

    def send6(b, ab, d):
        return y_hop(b, yrows(b, pos[1 - ab] - 1 + 2 * d), ycols(ab, pos[ab], d), 5, ab, d, 1 - ab)

    def land6(b, ab, d):
        return y_hop(b, yrows(b, pos[1 - ab] + 2), ycols(ab, pos[ab], d), 5, ab, d, 1 - ab)

    def send7(b, ab, d):
        return y_hop(b, yrows(b), ycols(ab, pos[ab]), 6, ab, d, ab)

    def land7(b, ab, d):
        return y_hop(b, yrows(b), ycols(ab, pos[ab] - 1 + 2 * d), 6, ab, d, ab)

    def send8(b, ab, d):
        return y_hop(b, yrows(b), ycols(ab, pos[ab] - 1 + 2 * d, d), 7, ab, d, ab)

    def land8(b, ab, d):
        return y_hop(b, yrows(b), ycols(ab, pos[ab] + 2, d), 7, ab, d, ab)

    sends = (send1, send2, send3, send4, send5, send6, send7, send8)

    def gpair(b, c):
        cols = pl.ds(pl.multiple_of(c * half, half), half)
        return pltpu.make_async_remote_copy(
            src_ref=ybuf.at[yrows(b), cols], dst_ref=ybuf.at[yrows(b), cols],
            send_sem=gpair_send.at[lax.rem(b, 2)], recv_sem=gpair_recv.at[b],
            device_id=dev(partner), device_id_type=pl.DeviceIdType.MESH)

    def kv_store(c):
        rows = pl.ds(pl.multiple_of(c * PAIR, PAIR), PAIR)
        slot = lax.rem(c, 2)
        return (pltpu.make_async_copy(kbuf.at[rows], k_hbm.at[rows], kvsem.at[slot, 0]),
                pltpu.make_async_copy(vbuf.at[rows], v_hbm.at[rows], kvsem.at[slot, 1]))

    def issue(send, b):
        for ab in (0, 1):
            for d in (0, 1):
                @pl.when(b >= 2)
                def _():
                    send(b - 2, ab, d).wait_send()
                send(b, ab, d).start()

    def attend(q, c, keys):
        ks = kbuf[pl.ds(0, keys), :]
        s = lax.dot_general(q, ks, (((1,), (1,)), ((), ())), preferred_element_type=F32)
        s = s * (1.0 / math.sqrt(HEAD_DIM))
        qpos = c * PAIR + lax.broadcasted_iota(jnp.int32, s.shape, 0)
        kpos = lax.broadcasted_iota(jnp.int32, s.shape, 1)
        s = jnp.where(kpos <= qpos, s, -1e30)
        top = jnp.max(s, axis=-1, keepdims=True)
        e = jnp.exp(s - top)
        probs = (e * (1.0 / jnp.sum(e, axis=-1, keepdims=True))).astype(BF16)
        o = jnp.dot(probs, vbuf[pl.ds(0, keys), :], preferred_element_type=F32)
        ombuf[:, pl.ds(0, HEAD_DIM)] = o.astype(BF16)

    def compute_a(c):
        slot = lax.rem(c, 2)
        for cp in x_load(c, slot):
            cp.wait()

        @pl.when(c + 1 < nblk // 2)
        def _():
            for cp in x_load(c + 1, 1 - slot):
                cp.start()

        for r in range(0, PAIR, 16):
            xr = xbuf[slot, pl.ds(r, 16), :].astype(F32)
            inv = lax.rsqrt(jnp.mean(xr * xr, axis=-1, keepdims=True) + NORM_EPS)
            for j in range(width // LANES):
                cols = slice(j * LANES, (j + 1) * LANES)
                abuf[pl.ds(r, 16), cols] = (xr[:, cols] * inv * g_ref[j:j + 1, :].astype(F32)).astype(BF16)

        @pl.when(c == 0)
        def _():
            for cp in w_loads[:3]:
                cp.wait()

        qkv = jnp.dot(abuf[...], wqkv[...], preferred_element_type=F32)
        cos_t = tabs[slot, 0]
        sin_t = tabs[slot, 1]

        def rope(z):
            return (z * cos_t + pltpu.roll(z, HEAD_DIM // 2, 1) * sin_t).astype(BF16)

        q = rope(qkv[:, :HEAD_DIM])
        rows = pl.ds(pl.multiple_of(c * PAIR, PAIR), PAIR)
        kbuf[rows, :] = rope(qkv[:, HEAD_DIM:2 * HEAD_DIM])
        vbuf[rows, :] = qkv[:, 2 * HEAD_DIM:].astype(BF16)

        @pl.when(c >= 2)
        def _():
            for cp in kv_store(c - 2):
                cp.wait()

        for cp in kv_store(c):
            cp.start()

        for n in range(tokens // KEYS):
            @pl.when(c * PAIR // KEYS == n)
            def _(n=n):
                attend(q, c, (n + 1) * KEYS)

    def compute_b(c):
        @pl.when(c == 0)
        def _():
            for cp in w_loads[3:]:
                cp.wait()

        gu = lax.dot_general(wgu[...], abuf[...], (((1,), (1,)), ((), ())), preferred_element_type=F32)
        gate, up = gu[:ff], gu[ff:]
        hidden = gate * jax.nn.sigmoid(gate) * up
        ombuf[:, pl.ds(HEAD_DIM, ff)] = hidden.T.astype(BF16)

        @pl.when(c >= 2)
        def _():
            pair_copy(2 * c - 4).wait_send()
            pair_copy(2 * c - 3).wait_send()

        om = ombuf[...]
        for c0 in range(0, width, OUT_TILE):
            cols = pl.ds(c0, OUT_TILE)
            share = jnp.dot(om, wod[:, cols], preferred_element_type=F32).astype(BF16)
            for i in (0, 1):
                part[lax.rem(2 * c + i, SLOTS), :, cols] = share[i * ROWS:(i + 1) * ROWS]
        pair_copy(2 * c).start()
        pair_copy(2 * c + 1).start()

    def add(dst, *srcs):
        total = dst[...].astype(F32)
        for s in srcs:
            total = total + s[...].astype(F32)
        dst[...] = total.astype(BF16)

    def both(f):
        for ab in (0, 1):
            for d in (0, 1):
                f(ab, d)

    def stage1(b):
        pair_copy(b).wait_recv()
        mine = pl.ds(pl.multiple_of(mine0, half), half)
        for r in range(0, ROWS, 32):
            add(quart.at[b, pl.ds(r, 32), :], part.at[lax.rem(b, SLOTS), pl.ds(r, 32), mine])
        issue(send1, b)

    def stage2(b):
        both(lambda ab, d: send1(b, ab, d).wait_recv())
        both(lambda ab, d: add(quart.at[b, :, qcols(ab, pos[ab] + 1 - 2 * d, d)], r1.at[lax.rem(b, SLOTS), ab, d]))
        issue(send2, b)

    def stage3(b):
        both(lambda ab, d: send2(b, ab, d).wait_recv())
        for ab in (0, 1):
            add(quart.at[b, :, qcols(ab, pos[ab])], r2.at[lax.rem(b, SLOTS), ab, 0], r2.at[lax.rem(b, SLOTS), ab, 1])
        issue(send3, b)

    def stage4(b):
        both(lambda ab, d: send3(b, ab, d).wait_recv())
        both(lambda ab, d: add(quart.at[b, brows(pos[1 - ab] + 1 - 2 * d), qcols(ab, pos[ab], d)], r3.at[b, ab, d]))
        issue(send4, b)

    def stage5(b):
        @pl.when(b == 0)
        def _():
            for c in res_loads:
                c.wait()

        both(lambda ab, d: send4(b, ab, d).wait_recv())
        for ab in (0, 1):
            p2 = pos[1 - ab]
            total = quart[b, brows(p2), qcols(ab, pos[ab])].astype(F32)
            total = total + r4[b, ab, 0].astype(F32) + r4[b, ab, 1].astype(F32)
            total = total + xres[ab, yrows(b, p2), :].astype(F32)
            ybuf[yrows(b, p2), ycols(ab, pos[ab])] = total.astype(BF16)
        issue(send5, b)

    def stage6(b):
        both(lambda ab, d: land5(b, ab, d).wait_recv())
        issue(send6, b)

    def stage7(b):
        both(lambda ab, d: land6(b, ab, d).wait_recv())
        issue(send7, b)

    def stage8(b):
        both(lambda ab, d: land7(b, ab, d).wait_recv())
        issue(send8, b)

    def stage9(b):
        both(lambda ab, d: land8(b, ab, d).wait_recv())

        @pl.when(b >= 2)
        def _():
            gpair(b - 2, core).wait_send()

        gpair(b, core).start()

    def stage10(b):
        gpair(b, 1 - core).wait_recv()

    stages = (stage1, stage2, stage3, stage4, stage5, stage6, stage7, stage8, stage9, stage10)

    pl.semaphore_wait(barrier, 5)

    @pl.loop(0, nblk + LAG[-1])
    def _(t):
        @pl.when((t < nblk) & (lax.rem(t, 2) == 0))
        def _():
            compute_a(t // 2)

        @pl.when((t < nblk) & (lax.rem(t, 2) == 1))
        def _():
            compute_b(t // 2)

        for lag, stage in zip(LAG, stages):
            b = t - lag

            @pl.when((b >= 0) & (b < nblk))
            def _(b=b, stage=stage):
                stage(b)

    for b in range(nblk - SLOTS, nblk):
        pair_copy(b).wait_send()
    for b in range(nblk - 2, nblk):
        for send in sends:
            both(lambda ab, d: send(b, ab, d).wait_send())
        gpair(b, core).wait_send()
    for c in range(nblk // 2 - 2, nblk // 2):
        for cp in kv_store(c):
            cp.wait()


def rope_tables(tokens):
    inv_freq = np.float32(ROPE_BASE) ** (-np.arange(0, HEAD_DIM, 2, dtype=np.float32) / np.float32(HEAD_DIM))
    angles = np.arange(tokens, dtype=np.float32)[:, None] * inv_freq[None, :]
    cos_half, sin_half = np.cos(angles), np.sin(angles)
    return np.stack([np.concatenate([cos_half, cos_half], axis=1), np.concatenate([-sin_half, sin_half], axis=1)])


def solution(mesh):
    tp_size = mesh.shape['tp']
    side = math.isqrt(tp_size // 2)

    def local_layer(x_in, g_norm, w_q, w_k, w_v, w_o, w_gate, w_up, w_down):
        tokens, width = x_in.shape
        kv_heads = w_k.shape[1] // HEAD_DIM
        ff = w_gate.shape[1]
        nblk = tokens // ROWS
        half = width // 2
        cw = half // 2 // side
        rw = ROWS // side
        any_spec = pl.BlockSpec(memory_space=pl.ANY)
        y, k, v = pl.pallas_call(
            functools.partial(layer_kernel, (tp_size, side, kv_heads)),
            out_shape=(pltpu.VMEM((tokens, width), BF16),
                       jax.ShapeDtypeStruct((tokens, HEAD_DIM), BF16),
                       jax.ShapeDtypeStruct((tokens, HEAD_DIM), BF16)),
            in_specs=[any_spec, pl.BlockSpec(memory_space=pltpu.VMEM)] + [any_spec] * 8,
            out_specs=(pl.BlockSpec(memory_space=pltpu.VMEM), any_spec, any_spec),
            scratch_shapes=[
                pltpu.VMEM((width, 3 * HEAD_DIM), BF16),
                pltpu.VMEM((2 * ff, width), BF16),
                pltpu.VMEM((HEAD_DIM + ff, width), BF16),
                pltpu.VMEM((2, PAIR, width), BF16),
                pltpu.VMEM((2, 2, PAIR, HEAD_DIM), F32),
                pltpu.VMEM((PAIR, width), BF16),
                pltpu.VMEM((PAIR, HEAD_DIM + ff), BF16),
                pltpu.VMEM((tokens, HEAD_DIM), BF16),
                pltpu.VMEM((tokens, HEAD_DIM), BF16),
                pltpu.VMEM((SLOTS, ROWS, width), BF16),
                pltpu.VMEM((nblk, ROWS, half), BF16),
                pltpu.VMEM((SLOTS, 2, 2, ROWS, cw // 2), BF16),
                pltpu.VMEM((SLOTS, 2, 2, ROWS, cw), BF16),
                pltpu.VMEM((nblk, 2, 2, rw, cw // 2), BF16),
                pltpu.VMEM((nblk, 2, 2, rw, cw), BF16),
                pltpu.VMEM((2, tokens, cw), BF16),
                pltpu.SemaphoreType.DMA((7,)),
                pltpu.SemaphoreType.DMA((2, 2)),
                pltpu.SemaphoreType.DMA((2,)),
                pltpu.SemaphoreType.DMA((2, 2)),
                pltpu.SemaphoreType.DMA((SLOTS,)),
                pltpu.SemaphoreType.DMA((nblk,)),
                pltpu.SemaphoreType.DMA((8, 2, 2, 2)),
                pltpu.SemaphoreType.DMA((8, 2, 2, nblk)),
                pltpu.SemaphoreType.DMA((2,)),
                pltpu.SemaphoreType.DMA((nblk,)),
            ],
            compiler_params=pltpu.CompilerParams(collective_id=0, has_side_effects=True, vmem_limit_bytes=46 * 1024 * 1024),
            name="layer",
        )(x_in, g_norm.reshape(width // LANES, LANES), jnp.asarray(rope_tables(tokens)), w_q, w_k, w_v, w_o, w_gate.T, w_up.T, w_down)
        return y, k.reshape(tokens, 1, HEAD_DIM), v.reshape(tokens, 1, HEAD_DIM)

    return jax.shard_map(local_layer, mesh=mesh, in_specs=(P('dp', None), P(None), P(None, 'tp'), P(None, None), P(None, None), P('tp', None), P(None, 'tp'), P(None, 'tp'), P('tp', None)), out_specs=(P('dp', None), P('dp', 'tp', None), P('dp', 'tp', None)), check_vma=False)
```

```python
import functools
import math
import jax
import jax.numpy as jnp
import numpy as np
from jax import lax
from jax.experimental import pallas as pl
from jax.experimental.pallas import tpu as pltpu
from jax.sharding import PartitionSpec as P

HEAD_DIM = 128
ROPE_BASE = 500000.0
NORM_EPS = 1e-5
LANES = 128
ROWS = 128
PAIR = 2 * ROWS
SLOTS = 4
RING = 4
KEYS = 512
OUT_TILE = 512
LAG = (2, 3, 4, 5, 6, 7, 8, 9, 10, 11)
FIRST = (6, 7, 8, 9, 10)
SECOND = (1, 2, 3, 4, 5)
BF16 = jnp.bfloat16
F32 = jnp.float32


def layer_kernel(cfg, x_hbm, g_ref, tab_hbm, wq_hbm, wk_hbm, wv_hbm, wo_hbm, wg_hbm, wu_hbm, wd_hbm,
                 ybuf, k_hbm, v_hbm,
                 wqkv, wall, wod, xbuf, tabs, abuf, atbuf, gbuf, qtbuf, ombuf, kbuf, vbuf, vtbuf, part, quart, r1, r2, r3, r4, xres,
                 wsem, xsem, ressem, kvsem, pair_send, pair_recv, ssem, rsem, gpair_send, gpair_recv):
    tokens, width = x_hbm.shape
    tp, side, kv_heads = cfg[:3]
    nblk = tokens // ROWS
    npair = tokens // PAIR
    half = width // 2
    quarter = half // 2
    cw = quarter // side
    ch = cw // 2
    rw = ROWS // side
    ff = wg_hbm.shape[0]

    me = lax.axis_index("tp")
    core = lax.rem(me, 2)
    px = lax.rem(me // 2, side)
    py = me // (2 * side)
    partner = me + 1 - 2 * core

    def wrap(p):
        return lax.rem(p + side, side)

    def at(y, x):
        return (wrap(y) * side + wrap(x)) * 2 + core

    near = (((at(py, px + 1)), (at(py, px - 1))), ((at(py + 1, px)), (at(py - 1, px))))
    pos = (px, py)

    def dev(d):
        return {"tp": d}

    barrier = pltpu.get_barrier_semaphore()
    for d in (partner, *near[0], *near[1]):
        pl.semaphore_signal(barrier, inc=1, device_id=dev(d), device_id_type=pl.DeviceIdType.MESH)

    head = lax.div(me * kv_heads, tp)
    kcol = pl.ds(pl.multiple_of(head * HEAD_DIM, HEAD_DIM), HEAD_DIM)
    mine0 = core * half
    res_col = [pl.multiple_of(mine0 + ab * quarter + pos[ab] * cw, cw) for ab in (0, 1)]

    def x_load(c, slot):
        rows = pl.ds(pl.multiple_of(c * PAIR, PAIR), PAIR)
        return (pltpu.make_async_copy(x_hbm.at[rows], xbuf, xsem.at[slot, 0]),
                pltpu.make_async_copy(tab_hbm.at[:, :, rows], tabs.at[slot], xsem.at[slot, 1]))

    w_loads = (
        pltpu.make_async_copy(wq_hbm, wqkv.at[0], wsem.at[0]),
        pltpu.make_async_copy(wk_hbm.at[:, kcol], wqkv.at[1], wsem.at[1]),
        pltpu.make_async_copy(wv_hbm.at[:, kcol], wqkv.at[2], wsem.at[2]),
        pltpu.make_async_copy(wg_hbm, wall.at[pl.ds(3 * HEAD_DIM, ff)], wsem.at[3]),
        pltpu.make_async_copy(wu_hbm, wall.at[pl.ds(3 * HEAD_DIM + ff, ff)], wsem.at[4]),
        pltpu.make_async_copy(wo_hbm, wod.at[pl.ds(0, HEAD_DIM)], wsem.at[5]),
        pltpu.make_async_copy(wd_hbm, wod.at[pl.ds(HEAD_DIM, ff)], wsem.at[6]),
    )
    for c in x_load(0, 0):
        c.start()
    for c in w_loads:
        c.start()
    res_loads = [pltpu.make_async_copy(x_hbm.at[:, pl.ds(res_col[ab], cw)], xres.at[ab], ressem.at[ab]) for ab in (0, 1)]
    for c in res_loads:
        c.start()
    kbuf[...] = jnp.zeros_like(kbuf)
    vtbuf[...] = jnp.zeros_like(vtbuf)

    def pair_copy(b):
        col = pl.multiple_of((1 - core) * half, half)
        return pltpu.make_async_remote_copy(
            src_ref=part.at[lax.rem(b, SLOTS), :, pl.ds(col, half)], dst_ref=quart.at[b],
            send_sem=pair_send.at[lax.rem(b, SLOTS)], recv_sem=pair_recv.at[b],
            device_id=dev(partner), device_id_type=pl.DeviceIdType.MESH)

    def hop(src, dst, st, b, ab, d, axis):
        return pltpu.make_async_remote_copy(
            src_ref=src, dst_ref=dst, send_sem=ssem.at[st, ab, d, lax.rem(b, 2)], recv_sem=rsem.at[st, ab, d, b],
            device_id=dev(near[axis][d]), device_id_type=pl.DeviceIdType.MESH)

    def qcols(ab, chunk, h=None):
        base = ab * quarter + wrap(chunk) * cw
        if h is None:
            return pl.ds(pl.multiple_of(base, cw), cw)
        return pl.ds(pl.multiple_of(base + h * ch, ch), ch)

    def ycols(ab, chunk, h=None):
        base = mine0 + ab * quarter + wrap(chunk) * cw
        if h is None:
            return pl.ds(pl.multiple_of(base, cw), cw)
        return pl.ds(pl.multiple_of(base + h * ch, ch), ch)

    def brows(chunk):
        return pl.ds(pl.multiple_of(wrap(chunk) * rw, rw), rw)

    def yrows(b, chunk=None):
        if chunk is None:
            return pl.ds(pl.multiple_of(b * ROWS, ROWS), ROWS)
        return pl.ds(pl.multiple_of(b * ROWS + wrap(chunk) * rw, rw), rw)

    def send1(b, ab, d):
        p = pos[ab]
        return hop(quart.at[b, :, qcols(ab, p + 2, d)], r1.at[lax.rem(b, RING), ab, d], 0, b, ab, d, ab)

    def send2(b, ab, d):
        p = pos[ab]
        return hop(quart.at[b, :, qcols(ab, p + 1 - 2 * d)], r2.at[lax.rem(b, RING), ab, d], 1, b, ab, d, ab)

    def send3(b, ab, d):
        p2 = pos[1 - ab]
        return hop(quart.at[b, brows(p2 + 2), qcols(ab, pos[ab], d)], r3.at[b, ab, d], 2, b, ab, d, 1 - ab)

    def send4(b, ab, d):
        p2 = pos[1 - ab]
        return hop(quart.at[b, brows(p2 + 1 - 2 * d), qcols(ab, pos[ab])], r4.at[b, ab, d], 3, b, ab, d, 1 - ab)

    def y_hop(b, rows, cols, st, ab, d, axis):
        return hop(ybuf.at[rows, cols], ybuf.at[rows, cols], st, b, ab, d, axis)

    def send5(b, ab, d):
        return y_hop(b, yrows(b, pos[1 - ab]), ycols(ab, pos[ab]), 4, ab, d, 1 - ab)

    def land5(b, ab, d):
        return y_hop(b, yrows(b, pos[1 - ab] - 1 + 2 * d), ycols(ab, pos[ab]), 4, ab, d, 1 - ab)

    def send6(b, ab, d):
        return y_hop(b, yrows(b, pos[1 - ab] - 1 + 2 * d), ycols(ab, pos[ab], d), 5, ab, d, 1 - ab)

    def land6(b, ab, d):
        return y_hop(b, yrows(b, pos[1 - ab] + 2), ycols(ab, pos[ab], d), 5, ab, d, 1 - ab)

    def send7(b, ab, d):
        return y_hop(b, yrows(b), ycols(ab, pos[ab]), 6, ab, d, ab)

    def land7(b, ab, d):
        return y_hop(b, yrows(b), ycols(ab, pos[ab] - 1 + 2 * d), 6, ab, d, ab)

    def send8(b, ab, d):
        return y_hop(b, yrows(b), ycols(ab, pos[ab] - 1 + 2 * d, d), 7, ab, d, ab)

    def land8(b, ab, d):
        return y_hop(b, yrows(b), ycols(ab, pos[ab] + 2, d), 7, ab, d, ab)

    sends = (send1, send2, send3, send4, send5, send6, send7, send8)

    def gpair(b, c):
        cols = pl.ds(pl.multiple_of(c * half, half), half)
        return pltpu.make_async_remote_copy(
            src_ref=ybuf.at[yrows(b), cols], dst_ref=ybuf.at[yrows(b), cols],
            send_sem=gpair_send.at[lax.rem(b, 2)], recv_sem=gpair_recv.at[b],
            device_id=dev(partner), device_id_type=pl.DeviceIdType.MESH)

    def kv_store(c):
        rows = pl.ds(pl.multiple_of(c * PAIR, PAIR), PAIR)
        slot = lax.rem(c, 2)
        return (pltpu.make_async_copy(kbuf.at[rows], k_hbm.at[rows], kvsem.at[slot, 0]),
                pltpu.make_async_copy(vbuf.at[slot], v_hbm.at[rows], kvsem.at[slot, 1]))

    def issue(send, b):
        @pl.when(b >= 2)
        def _():
            both(lambda ab, d: send(b - 2, ab, d).wait_send())

        both(lambda ab, d: send(b, ab, d).start())

    def attend(q_t, c, keys):
        s = jnp.dot(kbuf[pl.ds(0, keys), :], q_t, preferred_element_type=F32)
        edge = keys - KEYS
        tail = s[edge:]
        kpos = edge + lax.broadcasted_iota(jnp.int32, tail.shape, 0)
        qpos = c * PAIR + lax.broadcasted_iota(jnp.int32, tail.shape, 1)
        tail = jnp.where(kpos <= qpos, tail, -1e30)
        s = jnp.concatenate([s[:edge], tail], axis=0) if edge else tail
        top = jnp.max(s, axis=0, keepdims=True)
        e = jnp.exp2((s - top) * (math.log2(math.e) / math.sqrt(HEAD_DIM)))
        probs = (e * (1.0 / jnp.sum(e, axis=0, keepdims=True))).astype(BF16)
        o_t = jnp.dot(vtbuf[:, pl.ds(0, keys)], probs, preferred_element_type=F32)
        ombuf[:, pl.ds(0, HEAD_DIM)] = o_t.T.astype(BF16)

    def norm_rows(r):
        xr = xbuf[pl.ds(r, 16), :].astype(F32)
        inv = lax.rsqrt(jnp.mean(xr * xr, axis=-1, keepdims=True) + NORM_EPS)
        for j in range(width // LANES):
            cols = slice(j * LANES, (j + 1) * LANES)
            abuf[pl.ds(r, 16), cols] = (xr[:, cols] * inv * gbuf[:, cols]).astype(BF16)

    def turn(j):
        cols = pl.ds(j * LANES, LANES)
        atbuf[cols, :] = abuf[:, cols].T

    def first_norm():
        for j in range(width // LANES):
            gbuf[:, j * LANES:(j + 1) * LANES] = jnp.broadcast_to(g_ref[j:j + 1, :].astype(F32), (16, LANES))

        for cp in x_load(0, 0):
            cp.wait()
        @pl.loop(0, PAIR // 16)
        def _(i):
            norm_rows(pl.multiple_of(i * 16, 16))

        for cp in x_load(1, 1):
            cp.start()
        for j in range(width // LANES):
            turn(j)
        for cp in w_loads[:3]:
            cp.wait()
        for r in range(0, width, 512):
            for n in range(3):
                wall[pl.ds(n * HEAD_DIM, HEAD_DIM), pl.ds(r, 512)] = wqkv[n, pl.ds(r, 512), :].T

    def project(c):
        slot = lax.rem(c, 2)

        @pl.when(c + 1 < npair)
        def _():
            for cp in x_load(c + 1, 1 - slot):
                cp.wait()

        for r in range(0, PAIR // 2, 16):
            norm_rows(r)
        qkv = jnp.dot(wall[pl.ds(0, 3 * HEAD_DIM), :], atbuf[...], preferred_element_type=F32)
        cos_t = tabs[slot, 0]
        sin_t = tabs[slot, 1]

        def rope(z):
            lo, hi = z[:HEAD_DIM // 2], z[HEAD_DIM // 2:]
            return jnp.concatenate([lo * cos_t - hi * sin_t, hi * cos_t + lo * sin_t], axis=0)

        qtbuf[...] = rope(qkv[:HEAD_DIM]).astype(BF16)
        rows = pl.ds(pl.multiple_of(c * PAIR, PAIR), PAIR)
        kbuf[rows, :] = rope(qkv[HEAD_DIM:2 * HEAD_DIM]).T.astype(BF16)
        v_t = qkv[2 * HEAD_DIM:]
        vtbuf[:, rows] = v_t.astype(BF16)
        @pl.when(c >= 2)
        def _():
            for cp in kv_store(c - 2):
                cp.wait()

        vbuf[slot] = v_t.T.astype(BF16)
        for cp in kv_store(c):
            cp.start()

    def mix(c):
        @pl.when(c == 0)
        def _():
            for cp in w_loads[3:5]:
                cp.wait()

        for n in range(tokens // KEYS):
            @pl.when(c * PAIR // KEYS == n)
            def _(n=n):
                attend(qtbuf[...], c, (n + 1) * KEYS)
                gu = jnp.dot(wall[pl.ds(3 * HEAD_DIM, 2 * ff), :], atbuf[...], preferred_element_type=F32)
                gate, up = gu[:ff], gu[ff:]
                hidden = gate * jax.nn.sigmoid(gate) * up
                ombuf[:, pl.ds(HEAD_DIM, ff)] = hidden.T.astype(BF16)

    tiles = width // OUT_TILE

    def out_tiles(c, first, last):
        om = ombuf[...]
        for n in range(first, last):
            cols = pl.ds(n * OUT_TILE, OUT_TILE)
            share = jnp.dot(om, wod[:, cols], preferred_element_type=F32).astype(BF16)
            for i in (0, 1):
                part[lax.rem(2 * c + i, SLOTS), :, cols] = share[i * ROWS:(i + 1) * ROWS]
            early = tiles // 2
            if n < early:
                for r in range((early + n) * PAIR // tiles, (early + n + 1) * PAIR // tiles, 16):
                    norm_rows(r)
            else:
                late = width // LANES // (tiles - early)
                for j in range((n - early) * late, (n - early + 1) * late):
                    turn(j)

    def out_a(c):
        @pl.when(c == 0)
        def _():
            for cp in w_loads[5:]:
                cp.wait()

        @pl.when(c >= 2)
        def _():
            pair_copy(2 * c - 4).wait_send()
            pair_copy(2 * c - 3).wait_send()

        out_tiles(c, 0, tiles // 2)

        @pl.when(c + 2 < npair)
        def _():
            for cp in x_load(c + 2, lax.rem(c, 2)):
                cp.start()

    def out_b(c):
        out_tiles(c, tiles // 2, tiles)
        pair_copy(2 * c).start()
        pair_copy(2 * c + 1).start()

    def add(dst, *srcs):
        total = dst[...].astype(F32)
        for s in srcs:
            total = total + s[...].astype(F32)
        dst[...] = total.astype(BF16)

    def both(f):
        for ab in (0, 1):
            for d in (0, 1):
                f(ab, d)

    def stage1(b):
        pair_copy(b).wait_recv()
        mine = pl.ds(pl.multiple_of(mine0, half), half)
        for r in range(0, ROWS, 32):
            add(quart.at[b, pl.ds(r, 32), :], part.at[lax.rem(b, SLOTS), pl.ds(r, 32), mine])
        issue(send1, b)

    def stage2(b):
        both(lambda ab, d: send1(b, ab, d).wait_recv())
        both(lambda ab, d: add(quart.at[b, :, qcols(ab, pos[ab] + 1 - 2 * d, d)], r1.at[lax.rem(b, RING), ab, d]))
        issue(send2, b)

    def stage3(b):
        both(lambda ab, d: send2(b, ab, d).wait_recv())
        for ab in (0, 1):
            add(quart.at[b, :, qcols(ab, pos[ab])], r2.at[lax.rem(b, RING), ab, 0], r2.at[lax.rem(b, RING), ab, 1])
        issue(send3, b)

    def stage4(b):
        both(lambda ab, d: send3(b, ab, d).wait_recv())
        both(lambda ab, d: add(quart.at[b, brows(pos[1 - ab] + 1 - 2 * d), qcols(ab, pos[ab], d)], r3.at[b, ab, d]))
        issue(send4, b)

    def stage5(b):
        @pl.when(b == 0)
        def _():
            for c in res_loads:
                c.wait()

        both(lambda ab, d: send4(b, ab, d).wait_recv())
        for ab in (0, 1):
            p2 = pos[1 - ab]
            total = quart[b, brows(p2), qcols(ab, pos[ab])].astype(F32)
            total = total + r4[b, ab, 0].astype(F32) + r4[b, ab, 1].astype(F32)
            total = total + xres[ab, yrows(b, p2), :].astype(F32)
            ybuf[yrows(b, p2), ycols(ab, pos[ab])] = total.astype(BF16)
        issue(send5, b)

    def stage6(b):
        both(lambda ab, d: land5(b, ab, d).wait_recv())
        issue(send6, b)

    def stage7(b):
        both(lambda ab, d: land6(b, ab, d).wait_recv())
        issue(send7, b)

    def stage8(b):
        both(lambda ab, d: land7(b, ab, d).wait_recv())
        issue(send8, b)

    def stage9(b):
        both(lambda ab, d: land8(b, ab, d).wait_recv())

        @pl.when(b >= 2)
        def _():
            gpair(b - 2, core).wait_send()

        gpair(b, core).start()

    def stage10(b):
        gpair(b, 1 - core).wait_recv()

    stages = (stage1, stage2, stage3, stage4, stage5, stage6, stage7, stage8, stage9, stage10)

    first_norm()
    pl.semaphore_wait(barrier, 5)

    @pl.loop(0, nblk + LAG[-1])
    def _(t):
        def run(group):
            for n in group:
                b = t - LAG[n - 1]

                @pl.when((b >= 0) & (b < nblk))
                def _(b=b, n=n):
                    stages[n - 1](b)

        def work(parity, piece):
            @pl.when((t < nblk) & (lax.rem(t, 2) == parity))
            def _():
                piece(t // 2)

        work(0, project)
        work(1, out_a)
        run(FIRST)
        work(0, mix)
        work(1, out_b)
        run(SECOND)

    for b in range(nblk - SLOTS, nblk):
        pair_copy(b).wait_send()
    for b in range(nblk - 2, nblk):
        for send in sends:
            both(lambda ab, d: send(b, ab, d).wait_send())
        gpair(b, core).wait_send()
    for c in range(nblk // 2 - 2, nblk // 2):
        for cp in kv_store(c):
            cp.wait()


def rope_tables(tokens):
    inv_freq = np.float32(ROPE_BASE) ** (-np.arange(0, HEAD_DIM, 2, dtype=np.float32) / np.float32(HEAD_DIM))
    angles = np.arange(tokens, dtype=np.float32)[:, None] * inv_freq[None, :]
    return np.stack([np.cos(angles).T, np.sin(angles).T])


def solution(mesh):
    tp_size = mesh.shape['tp']
    side = math.isqrt(tp_size // 2)

    def local_layer(x_in, g_norm, w_q, w_k, w_v, w_o, w_gate, w_up, w_down):
        tokens, width = x_in.shape
        kv_heads = w_k.shape[1] // HEAD_DIM
        ff = w_gate.shape[1]
        nblk = tokens // ROWS
        half = width // 2
        cw = half // 2 // side
        rw = ROWS // side
        any_spec = pl.BlockSpec(memory_space=pl.ANY)
        y, k, v = pl.pallas_call(
            functools.partial(layer_kernel, (tp_size, side, kv_heads)),
            out_shape=(pltpu.VMEM((tokens, width), BF16),
                       jax.ShapeDtypeStruct((tokens, HEAD_DIM), BF16),
                       jax.ShapeDtypeStruct((tokens, HEAD_DIM), BF16)),
            in_specs=[any_spec, pl.BlockSpec(memory_space=pltpu.VMEM)] + [any_spec] * 8,
            out_specs=(pl.BlockSpec(memory_space=pltpu.VMEM), any_spec, any_spec),
            scratch_shapes=[
                pltpu.VMEM((3, width, HEAD_DIM), BF16),
                pltpu.VMEM((3 * HEAD_DIM + 2 * ff, width), BF16),
                pltpu.VMEM((HEAD_DIM + ff, width), BF16),
                pltpu.VMEM((PAIR, width), BF16),
                pltpu.VMEM((2, 2, HEAD_DIM // 2, PAIR), F32),
                pltpu.VMEM((PAIR, width), BF16),
                pltpu.VMEM((width, PAIR), BF16),
                pltpu.VMEM((16, width), F32),
                pltpu.VMEM((HEAD_DIM, PAIR), BF16),
                pltpu.VMEM((PAIR, HEAD_DIM + ff), BF16),
                pltpu.VMEM((tokens, HEAD_DIM), BF16),
                pltpu.VMEM((2, PAIR, HEAD_DIM), BF16),
                pltpu.VMEM((HEAD_DIM, tokens), BF16),
                pltpu.VMEM((SLOTS, ROWS, width), BF16),
                pltpu.VMEM((nblk, ROWS, half), BF16),
                pltpu.VMEM((RING, 2, 2, ROWS, cw // 2), BF16),
                pltpu.VMEM((RING, 2, 2, ROWS, cw), BF16),
                pltpu.VMEM((nblk, 2, 2, rw, cw // 2), BF16),
                pltpu.VMEM((nblk, 2, 2, rw, cw), BF16),
                pltpu.VMEM((2, tokens, cw), BF16),
                pltpu.SemaphoreType.DMA((7,)),
                pltpu.SemaphoreType.DMA((2, 2)),
                pltpu.SemaphoreType.DMA((2,)),
                pltpu.SemaphoreType.DMA((2, 2)),
                pltpu.SemaphoreType.DMA((SLOTS,)),
                pltpu.SemaphoreType.DMA((nblk,)),
                pltpu.SemaphoreType.DMA((8, 2, 2, 2)),
                pltpu.SemaphoreType.DMA((8, 2, 2, nblk)),
                pltpu.SemaphoreType.DMA((2,)),
                pltpu.SemaphoreType.DMA((nblk,)),
            ],
            compiler_params=pltpu.CompilerParams(collective_id=0, has_side_effects=True, vmem_limit_bytes=47 * 1024 * 1024),
            name="layer",
        )(x_in, g_norm.reshape(width // LANES, LANES), jnp.asarray(rope_tables(tokens)), w_q, w_k, w_v, w_o, w_gate.T, w_up.T, w_down)
        return y, k.reshape(tokens, 1, HEAD_DIM), v.reshape(tokens, 1, HEAD_DIM)

    return jax.shard_map(local_layer, mesh=mesh, in_specs=(P('dp', None), P(None), P(None, 'tp'), P(None, None), P(None, None), P('tp', None), P(None, 'tp'), P(None, 'tp'), P('tp', None)), out_specs=(P('dp', None), P('dp', 'tp', None), P('dp', 'tp', None)), check_vma=False)
```

```python
import functools
import math
import jax
import jax.numpy as jnp
import numpy as np
from jax import lax
from jax.experimental import pallas as pl
from jax.experimental.pallas import tpu as pltpu
from jax.sharding import PartitionSpec as P

HEAD_DIM = 128
ROPE_BASE = 500000.0
NORM_EPS = 1e-5
LANES = 128
ROWS = 128
PAIR = 2 * ROWS
SLOTS = 2
RING = 4
KEYS = 512
OUT_TILE = 512
LAG = (2, 3, 4, 5, 6, 7, 8, 9, 10, 11)
BF16 = jnp.bfloat16
F32 = jnp.float32


def layer_kernel(cfg, x_hbm, g_ref, tab_hbm, wq_hbm, wk_hbm, wv_hbm, wo_hbm, wg_hbm, wu_hbm, wd_hbm,
                 ybuf, k_hbm, v_hbm,
                 wqkv, wall, wod, xbuf, tabs, abuf, atbuf, gbuf, qtbuf, silu, ombuf, kbuf, vbuf, vtbuf, part, quart, r1, r2, r3, r4, xres,
                 wsem, xsem, ressem, kvsem, pair_send, pair_recv, ssem, rsem, gpair_send, gpair_recv):
    tokens, width = x_hbm.shape
    tp, side, kv_heads = cfg[:3]
    nblk = tokens // ROWS
    npair = tokens // PAIR
    half = width // 2
    quarter = half // 2
    cw = quarter // side
    ch = cw // 2
    rw = ROWS // side
    ff = wg_hbm.shape[0]

    me = lax.axis_index("tp")
    core = lax.rem(me, 2)
    px = lax.rem(me // 2, side)
    py = me // (2 * side)
    partner = me + 1 - 2 * core

    def wrap(p):
        return lax.rem(p + side, side)

    def at(y, x):
        return (wrap(y) * side + wrap(x)) * 2 + core

    near = (((at(py, px + 1)), (at(py, px - 1))), ((at(py + 1, px)), (at(py - 1, px))))
    pos = (px, py)

    def dev(d):
        return {"tp": d}

    barrier = pltpu.get_barrier_semaphore()
    for d in (partner, *near[0], *near[1]):
        pl.semaphore_signal(barrier, inc=1, device_id=dev(d), device_id_type=pl.DeviceIdType.MESH)

    head = lax.div(me * kv_heads, tp)
    kcol = pl.ds(pl.multiple_of(head * HEAD_DIM, HEAD_DIM), HEAD_DIM)
    mine0 = core * half
    res_col = [pl.multiple_of(mine0 + ab * quarter + pos[ab] * cw, cw) for ab in (0, 1)]

    def x_load(c, slot):
        rows = pl.ds(pl.multiple_of(c * PAIR, PAIR), PAIR)
        return (pltpu.make_async_copy(x_hbm.at[rows], xbuf, xsem.at[slot, 0]),
                pltpu.make_async_copy(tab_hbm.at[:, :, rows], tabs.at[slot], xsem.at[slot, 1]))

    w_loads = (
        pltpu.make_async_copy(wq_hbm, wqkv.at[0], wsem.at[0]),
        pltpu.make_async_copy(wk_hbm.at[:, kcol], wqkv.at[1], wsem.at[1]),
        pltpu.make_async_copy(wv_hbm.at[:, kcol], wqkv.at[2], wsem.at[2]),
        pltpu.make_async_copy(wg_hbm, wall.at[pl.ds(3 * HEAD_DIM, ff)], wsem.at[3]),
        pltpu.make_async_copy(wu_hbm, wall.at[pl.ds(3 * HEAD_DIM + ff, ff)], wsem.at[4]),
        pltpu.make_async_copy(wo_hbm, wod.at[pl.ds(0, HEAD_DIM)], wsem.at[5]),
        pltpu.make_async_copy(wd_hbm, wod.at[pl.ds(HEAD_DIM, ff)], wsem.at[6]),
    )
    for c in x_load(0, 0):
        c.start()
    for c in w_loads:
        c.start()
    res_loads = [pltpu.make_async_copy(x_hbm.at[:, pl.ds(res_col[ab], cw)], xres.at[ab], ressem.at[ab]) for ab in (0, 1)]
    for c in res_loads:
        c.start()
    kbuf[...] = jnp.zeros_like(kbuf)
    vtbuf[...] = jnp.zeros_like(vtbuf)

    def pair_copy(b):
        col = pl.multiple_of((1 - core) * half, half)
        return pltpu.make_async_remote_copy(
            src_ref=part.at[lax.rem(b, SLOTS), :, pl.ds(col, half)], dst_ref=quart.at[b],
            send_sem=pair_send.at[lax.rem(b, SLOTS)], recv_sem=pair_recv.at[b],
            device_id=dev(partner), device_id_type=pl.DeviceIdType.MESH)

    def hop(src, dst, st, b, ab, d, axis):
        return pltpu.make_async_remote_copy(
            src_ref=src, dst_ref=dst, send_sem=ssem.at[st, ab, d, lax.rem(b, 2)], recv_sem=rsem.at[st, ab, d, b],
            device_id=dev(near[axis][d]), device_id_type=pl.DeviceIdType.MESH)

    def qcols(ab, chunk, h=None):
        base = ab * quarter + wrap(chunk) * cw
        if h is None:
            return pl.ds(pl.multiple_of(base, cw), cw)
        return pl.ds(pl.multiple_of(base + h * ch, ch), ch)

    def ycols(ab, chunk, h=None):
        base = mine0 + ab * quarter + wrap(chunk) * cw
        if h is None:
            return pl.ds(pl.multiple_of(base, cw), cw)
        return pl.ds(pl.multiple_of(base + h * ch, ch), ch)

    def brows(chunk):
        return pl.ds(pl.multiple_of(wrap(chunk) * rw, rw), rw)

    def yrows(b, chunk=None):
        if chunk is None:
            return pl.ds(pl.multiple_of(b * ROWS, ROWS), ROWS)
        return pl.ds(pl.multiple_of(b * ROWS + wrap(chunk) * rw, rw), rw)

    def send1(b, ab, d):
        p = pos[ab]
        return hop(quart.at[b, :, qcols(ab, p + 2, d)], r1.at[lax.rem(b, RING), ab, d], 0, b, ab, d, ab)

    def send2(b, ab, d):
        p = pos[ab]
        return hop(quart.at[b, :, qcols(ab, p + 1 - 2 * d)], r2.at[lax.rem(b, RING), ab, d], 1, b, ab, d, ab)

    def send3(b, ab, d):
        p2 = pos[1 - ab]
        return hop(quart.at[b, brows(p2 + 2), qcols(ab, pos[ab], d)], r3.at[b, ab, d], 2, b, ab, d, 1 - ab)

    def send4(b, ab, d):
        p2 = pos[1 - ab]
        return hop(quart.at[b, brows(p2 + 1 - 2 * d), qcols(ab, pos[ab])], r4.at[b, ab, d], 3, b, ab, d, 1 - ab)

    def y_hop(b, rows, cols, st, ab, d, axis):
        return hop(ybuf.at[rows, cols], ybuf.at[rows, cols], st, b, ab, d, axis)

    def send5(b, ab, d):
        return y_hop(b, yrows(b, pos[1 - ab]), ycols(ab, pos[ab]), 4, ab, d, 1 - ab)

    def land5(b, ab, d):
        return y_hop(b, yrows(b, pos[1 - ab] - 1 + 2 * d), ycols(ab, pos[ab]), 4, ab, d, 1 - ab)

    def send6(b, ab, d):
        return y_hop(b, yrows(b, pos[1 - ab] - 1 + 2 * d), ycols(ab, pos[ab], d), 5, ab, d, 1 - ab)

    def land6(b, ab, d):
        return y_hop(b, yrows(b, pos[1 - ab] + 2), ycols(ab, pos[ab], d), 5, ab, d, 1 - ab)

    def send7(b, ab, d):
        return y_hop(b, yrows(b), ycols(ab, pos[ab]), 6, ab, d, ab)

    def land7(b, ab, d):
        return y_hop(b, yrows(b), ycols(ab, pos[ab] - 1 + 2 * d), 6, ab, d, ab)

    def send8(b, ab, d):
        return y_hop(b, yrows(b), ycols(ab, pos[ab] - 1 + 2 * d, d), 7, ab, d, ab)

    def land8(b, ab, d):
        return y_hop(b, yrows(b), ycols(ab, pos[ab] + 2, d), 7, ab, d, ab)

    sends = (send1, send2, send3, send4, send5, send6, send7, send8)

    def gpair(b, c):
        cols = pl.ds(pl.multiple_of(c * half, half), half)
        return pltpu.make_async_remote_copy(
            src_ref=ybuf.at[yrows(b), cols], dst_ref=ybuf.at[yrows(b), cols],
            send_sem=gpair_send.at[lax.rem(b, 2)], recv_sem=gpair_recv.at[b],
            device_id=dev(partner), device_id_type=pl.DeviceIdType.MESH)

    def wait_all(copies):
        for cp in copies:
            cp.wait()

    def kv_store(c):
        rows = pl.ds(pl.multiple_of(c * PAIR, PAIR), PAIR)
        slot = lax.rem(c, 2)
        return (pltpu.make_async_copy(kbuf.at[rows], k_hbm.at[rows], kvsem.at[slot, 0]),
                pltpu.make_async_copy(vbuf.at[slot], v_hbm.at[rows], kvsem.at[slot, 1]))

    def issue(send, b):
        @pl.when(b >= 2)
        def _():
            both(lambda ab, d: send(b - 2, ab, d).wait_send())

        both(lambda ab, d: send(b, ab, d).start())

    def attend(q_t, c, keys):
        s = jnp.dot(kbuf[pl.ds(0, keys), :], q_t, preferred_element_type=F32)
        edge = keys - KEYS
        tail = s[edge:]
        kpos = edge + lax.broadcasted_iota(jnp.int32, tail.shape, 0)
        qpos = c * PAIR + lax.broadcasted_iota(jnp.int32, tail.shape, 1)
        tail = jnp.where(kpos <= qpos, tail, -1e30)
        s = jnp.concatenate([s[:edge], tail], axis=0) if edge else tail
        top = jnp.max(s, axis=0, keepdims=True)
        e = jnp.exp2((s - top) * (math.log2(math.e) / math.sqrt(HEAD_DIM)))
        probs = (e * (1.0 / jnp.sum(e, axis=0, keepdims=True))).astype(BF16)
        o_t = jnp.dot(vtbuf[:, pl.ds(0, keys)], probs, preferred_element_type=F32)
        ombuf[:, pl.ds(0, HEAD_DIM)] = o_t.T.astype(BF16)

    def norm_rows(r):
        rows = pl.ds(r, 16)
        sums = [jnp.zeros((16, LANES), F32)] * 2
        for j in range(width // LANES):
            xr = xbuf[rows, pl.ds(j * LANES, LANES)].astype(F32)
            sums[j % 2] = sums[j % 2] + xr * xr
        mean = jnp.sum(sums[0] + sums[1], axis=-1, keepdims=True) * (1.0 / width)
        inv = jnp.broadcast_to(lax.rsqrt(mean + NORM_EPS), (16, LANES))
        for j in range(width // LANES):
            cols = pl.ds(j * LANES, LANES)
            abuf[rows, cols] = (xbuf[rows, cols].astype(F32) * inv * gbuf[:, cols]).astype(BF16)

    def turn(j):
        cols = pl.ds(j * LANES, LANES)
        atbuf[cols, :] = abuf[:, cols].T

    def first_norm():
        for j in range(width // LANES):
            gbuf[:, j * LANES:(j + 1) * LANES] = jnp.broadcast_to(g_ref[j:j + 1, :].astype(F32), (16, LANES))

        for cp in x_load(0, 0):
            cp.wait()
        @pl.loop(0, PAIR // 16)
        def _(i):
            norm_rows(pl.multiple_of(i * 16, 16))

        for cp in x_load(1, 1):
            cp.start()
        for j in range(width // LANES):
            turn(j)
        for cp in w_loads[:3]:
            cp.wait()
        for r in range(0, width, 512):
            for n in range(3):
                wall[pl.ds(n * HEAD_DIM, HEAD_DIM), pl.ds(r, 512)] = wqkv[n, pl.ds(r, 512), :].T

    def project(c):
        slot = lax.rem(c, 2)
        qkv = jnp.dot(wall[pl.ds(0, 3 * HEAD_DIM), :], atbuf[...], preferred_element_type=F32)
        cos_t = tabs[slot, 0]
        sin_t = tabs[slot, 1]

        def rope(z):
            lo, hi = z[:HEAD_DIM // 2], z[HEAD_DIM // 2:]
            return jnp.concatenate([lo * cos_t - hi * sin_t, hi * cos_t + lo * sin_t], axis=0)

        qtbuf[...] = rope(qkv[:HEAD_DIM]).astype(BF16)
        rows = pl.ds(pl.multiple_of(c * PAIR, PAIR), PAIR)
        kbuf[rows, :] = rope(qkv[HEAD_DIM:2 * HEAD_DIM]).T.astype(BF16)
        v_t = qkv[2 * HEAD_DIM:]
        vtbuf[:, rows] = v_t.astype(BF16)
        @pl.when(c >= 2)
        def _():
            for cp in kv_store(c - 2):
                cp.wait()

        vbuf[slot] = v_t.T.astype(BF16)
        for cp in kv_store(c):
            cp.start()

    def open_gate(c):
        @pl.when(c == 0)
        def _():
            wait_all(w_loads[3:4])

        gate = jnp.dot(wall[pl.ds(3 * HEAD_DIM, ff), :], atbuf[...], preferred_element_type=F32)
        silu[...] = gate * jax.nn.sigmoid(gate)

    def mix(c):
        @pl.when(c == 0)
        def _():
            wait_all(w_loads[4:])

        for n in range(tokens // KEYS):
            @pl.when(c * PAIR // KEYS == n)
            def _(n=n):
                attend(qtbuf[...], c, (n + 1) * KEYS)
                up = jnp.dot(wall[pl.ds(3 * HEAD_DIM + ff, ff), :], atbuf[...], preferred_element_type=F32)
                ombuf[:, pl.ds(HEAD_DIM, ff)] = (silu[...] * up).T.astype(BF16)

    tiles = width // OUT_TILE

    def share_out(b, i):
        @pl.when(b >= SLOTS)
        def _():
            pair_copy(b - SLOTS).wait_send()

        om = ombuf[pl.ds(i * ROWS, ROWS), :]
        for n in range(tiles):
            cols = pl.ds(n * OUT_TILE, OUT_TILE)
            part[lax.rem(b, SLOTS), :, cols] = jnp.dot(om, wod[:, cols], preferred_element_type=F32).astype(BF16)
            if i == 0:
                for r in range(n * PAIR // tiles, (n + 1) * PAIR // tiles, 16):
                    norm_rows(r)
            else:
                for j in range(n * width // LANES // tiles, (n + 1) * width // LANES // tiles):
                    turn(j)
        pair_copy(b).start()

    def add(dst, *srcs):
        total = dst[...].astype(F32)
        for s in srcs:
            total = total + s[...].astype(F32)
        dst[...] = total.astype(BF16)

    def both(f):
        for ab in (0, 1):
            for d in (0, 1):
                f(ab, d)

    def stage1(b):
        pair_copy(b).wait_recv()
        mine = pl.ds(pl.multiple_of(mine0, half), half)
        for r in range(0, ROWS, 32):
            add(quart.at[b, pl.ds(r, 32), :], part.at[lax.rem(b, SLOTS), pl.ds(r, 32), mine])
        issue(send1, b)

    def stage2(b):
        both(lambda ab, d: send1(b, ab, d).wait_recv())
        both(lambda ab, d: add(quart.at[b, :, qcols(ab, pos[ab] + 1 - 2 * d, d)], r1.at[lax.rem(b, RING), ab, d]))
        issue(send2, b)

    def stage3(b):
        both(lambda ab, d: send2(b, ab, d).wait_recv())
        for ab in (0, 1):
            add(quart.at[b, :, qcols(ab, pos[ab])], r2.at[lax.rem(b, RING), ab, 0], r2.at[lax.rem(b, RING), ab, 1])
        issue(send3, b)

    def stage4(b):
        both(lambda ab, d: send3(b, ab, d).wait_recv())
        both(lambda ab, d: add(quart.at[b, brows(pos[1 - ab] + 1 - 2 * d), qcols(ab, pos[ab], d)], r3.at[b, ab, d]))
        issue(send4, b)

    def stage5(b):
        @pl.when(b == 0)
        def _():
            for c in res_loads:
                c.wait()

        both(lambda ab, d: send4(b, ab, d).wait_recv())
        for ab in (0, 1):
            p2 = pos[1 - ab]
            total = quart[b, brows(p2), qcols(ab, pos[ab])].astype(F32)
            total = total + r4[b, ab, 0].astype(F32) + r4[b, ab, 1].astype(F32)
            total = total + xres[ab, yrows(b, p2), :].astype(F32)
            ybuf[yrows(b, p2), ycols(ab, pos[ab])] = total.astype(BF16)
        issue(send5, b)

    def stage6(b):
        both(lambda ab, d: land5(b, ab, d).wait_recv())
        issue(send6, b)

    def stage7(b):
        both(lambda ab, d: land6(b, ab, d).wait_recv())
        issue(send7, b)

    def stage8(b):
        both(lambda ab, d: land7(b, ab, d).wait_recv())
        issue(send8, b)

    def stage9(b):
        both(lambda ab, d: land8(b, ab, d).wait_recv())

        @pl.when(b >= 2)
        def _():
            gpair(b - 2, core).wait_send()

        gpair(b, core).start()

    def stage10(b):
        gpair(b, 1 - core).wait_recv()

    stages = (stage1, stage2, stage3, stage4, stage5, stage6, stage7, stage8, stage9, stage10)

    first_norm()
    pl.semaphore_wait(barrier, 5)

    @pl.loop(0, nblk + LAG[-1])
    def _(t):
        even = lax.rem(t, 2) == 0

        @pl.when(even & (t >= 2) & (t <= nblk))
        def _():
            share_out(t - 1, 1)

        @pl.when(even & (t < nblk))
        def _():
            project(t // 2)
            open_gate(t // 2)

        @pl.when((t < nblk) & (lax.rem(t, 2) == 1))
        def _():
            c = t // 2
            mix(c)

            @pl.when(c + 1 < npair)
            def _():
                wait_all(x_load(c + 1, lax.rem(c + 1, 2)))

            share_out(t - 1, 0)

            @pl.when(c + 2 < npair)
            def _():
                for cp in x_load(c + 2, lax.rem(c, 2)):
                    cp.start()

        for lag, stage in zip(LAG, stages):
            b = t - lag

            @pl.when((b >= 0) & (b < nblk))
            def _(b=b, stage=stage):
                stage(b)

    for b in range(nblk - SLOTS, nblk):
        pair_copy(b).wait_send()
    for b in range(nblk - 2, nblk):
        for send in sends:
            both(lambda ab, d: send(b, ab, d).wait_send())
        gpair(b, core).wait_send()
    for c in range(nblk // 2 - 2, nblk // 2):
        for cp in kv_store(c):
            cp.wait()


def rope_tables(tokens):
    inv_freq = np.float32(ROPE_BASE) ** (-np.arange(0, HEAD_DIM, 2, dtype=np.float32) / np.float32(HEAD_DIM))
    angles = np.arange(tokens, dtype=np.float32)[:, None] * inv_freq[None, :]
    return np.stack([np.cos(angles).T, np.sin(angles).T])


def solution(mesh):
    tp_size = mesh.shape['tp']
    side = math.isqrt(tp_size // 2)

    def local_layer(x_in, g_norm, w_q, w_k, w_v, w_o, w_gate, w_up, w_down):
        tokens, width = x_in.shape
        kv_heads = w_k.shape[1] // HEAD_DIM
        ff = w_gate.shape[1]
        nblk = tokens // ROWS
        half = width // 2
        cw = half // 2 // side
        rw = ROWS // side
        any_spec = pl.BlockSpec(memory_space=pl.ANY)
        y, k, v = pl.pallas_call(
            functools.partial(layer_kernel, (tp_size, side, kv_heads)),
            out_shape=(pltpu.VMEM((tokens, width), BF16),
                       jax.ShapeDtypeStruct((tokens, HEAD_DIM), BF16),
                       jax.ShapeDtypeStruct((tokens, HEAD_DIM), BF16)),
            in_specs=[any_spec, pl.BlockSpec(memory_space=pltpu.VMEM)] + [any_spec] * 8,
            out_specs=(pl.BlockSpec(memory_space=pltpu.VMEM), any_spec, any_spec),
            scratch_shapes=[
                pltpu.VMEM((3, width, HEAD_DIM), BF16),
                pltpu.VMEM((3 * HEAD_DIM + 2 * ff, width), BF16),
                pltpu.VMEM((HEAD_DIM + ff, width), BF16),
                pltpu.VMEM((PAIR, width), BF16),
                pltpu.VMEM((2, 2, HEAD_DIM // 2, PAIR), F32),
                pltpu.VMEM((PAIR, width), BF16),
                pltpu.VMEM((width, PAIR), BF16),
                pltpu.VMEM((16, width), F32),
                pltpu.VMEM((HEAD_DIM, PAIR), BF16),
                pltpu.VMEM((ff, PAIR), F32),
                pltpu.VMEM((PAIR, HEAD_DIM + ff), BF16),
                pltpu.VMEM((tokens, HEAD_DIM), BF16),
                pltpu.VMEM((2, PAIR, HEAD_DIM), BF16),
                pltpu.VMEM((HEAD_DIM, tokens), BF16),
                pltpu.VMEM((SLOTS, ROWS, width), BF16),
                pltpu.VMEM((nblk, ROWS, half), BF16),
                pltpu.VMEM((RING, 2, 2, ROWS, cw // 2), BF16),
                pltpu.VMEM((RING, 2, 2, ROWS, cw), BF16),
                pltpu.VMEM((nblk, 2, 2, rw, cw // 2), BF16),
                pltpu.VMEM((nblk, 2, 2, rw, cw), BF16),
                pltpu.VMEM((2, tokens, cw), BF16),
                pltpu.SemaphoreType.DMA((7,)),
                pltpu.SemaphoreType.DMA((2, 2)),
                pltpu.SemaphoreType.DMA((2,)),
                pltpu.SemaphoreType.DMA((2, 2)),
                pltpu.SemaphoreType.DMA((SLOTS,)),
                pltpu.SemaphoreType.DMA((nblk,)),
                pltpu.SemaphoreType.DMA((8, 2, 2, 2)),
                pltpu.SemaphoreType.DMA((8, 2, 2, nblk)),
                pltpu.SemaphoreType.DMA((2,)),
                pltpu.SemaphoreType.DMA((nblk,)),
            ],
            compiler_params=pltpu.CompilerParams(collective_id=0, has_side_effects=True, vmem_limit_bytes=47 * 1024 * 1024),
            name="layer",
        )(x_in, g_norm.reshape(width // LANES, LANES), jnp.asarray(rope_tables(tokens)), w_q, w_k, w_v, w_o, w_gate.T, w_up.T, w_down)
        return y, k.reshape(tokens, 1, HEAD_DIM), v.reshape(tokens, 1, HEAD_DIM)

    return jax.shard_map(local_layer, mesh=mesh, in_specs=(P('dp', None), P(None), P(None, 'tp'), P(None, None), P(None, None), P('tp', None), P(None, 'tp'), P(None, 'tp'), P('tp', None)), out_specs=(P('dp', None), P('dp', 'tp', None), P('dp', 'tp', None)), check_vma=False)
```

```python
import functools
import math
import jax
import jax.numpy as jnp
import numpy as np
from jax import lax
from jax.experimental import pallas as pl
from jax.experimental.pallas import tpu as pltpu
from jax.sharding import PartitionSpec as P

HEAD_DIM = 128
ROPE_BASE = 500000.0
NORM_EPS = 1e-5
LANES = 128
ROWS = 128
SLOTS = 2
RING = 4
KEYS = 512
OUT_TILE = 512
LAG = (1, 2, 3, 4, 5, 6, 7, 8, 9, 10)
BF16 = jnp.bfloat16
F32 = jnp.float32


def layer_kernel(cfg, x_hbm, g_ref, tab_hbm, wq_hbm, wk_hbm, wv_hbm, wo_hbm, wg_hbm, wu_hbm, wd_hbm,
                 ybuf, k_hbm, v_hbm,
                 wall, wgu, wod, xbuf, tabs, abuf, gbuf, ombuf, kbuf, vbuf, part, quart, r1, r2, r3, r4, xres,
                 wsem, xsem, ressem, kvsem, pair_send, pair_recv, ssem, rsem, gpair_send, gpair_recv):
    tokens, width = x_hbm.shape
    tp, side, kv_heads = cfg[:3]
    nblk = tokens // ROWS
    half = width // 2
    quarter = half // 2
    cw = quarter // side
    ch = cw // 2
    rw = ROWS // side
    ff = wg_hbm.shape[0]

    me = lax.axis_index("tp")
    core = lax.rem(me, 2)
    px = lax.rem(me // 2, side)
    py = me // (2 * side)
    partner = me + 1 - 2 * core

    def wrap(p):
        return lax.rem(p + side, side)

    def at(y, x):
        return (wrap(y) * side + wrap(x)) * 2 + core

    near = (((at(py, px + 1)), (at(py, px - 1))), ((at(py + 1, px)), (at(py - 1, px))))
    pos = (px, py)

    def dev(d):
        return {"tp": d}

    barrier = pltpu.get_barrier_semaphore()
    for d in (partner, *near[0], *near[1]):
        pl.semaphore_signal(barrier, inc=1, device_id=dev(d), device_id_type=pl.DeviceIdType.MESH)

    head = lax.div(me * kv_heads, tp)
    kcol = pl.ds(pl.multiple_of(head * HEAD_DIM, HEAD_DIM), HEAD_DIM)
    mine0 = core * half
    res_col = [pl.multiple_of(mine0 + ab * quarter + pos[ab] * cw, cw) for ab in (0, 1)]

    def x_load(b):
        rows = pl.ds(pl.multiple_of(b * ROWS, ROWS), ROWS)
        slot = lax.rem(b, 2)
        return (pltpu.make_async_copy(x_hbm.at[rows], xbuf, xsem.at[slot, 0]),
                pltpu.make_async_copy(tab_hbm.at[:, rows], tabs.at[slot], xsem.at[slot, 1]))

    w_loads = (
        pltpu.make_async_copy(wg_hbm, wgu.at[pl.ds(0, ff)], wsem.at[0]),
        pltpu.make_async_copy(wu_hbm, wgu.at[pl.ds(ff, ff)], wsem.at[1]),
        pltpu.make_async_copy(wq_hbm, wall.at[:, pl.ds(0, HEAD_DIM)], wsem.at[2]),
        pltpu.make_async_copy(wk_hbm.at[:, kcol], wall.at[:, pl.ds(HEAD_DIM, HEAD_DIM)], wsem.at[3]),
        pltpu.make_async_copy(wv_hbm.at[:, kcol], wall.at[:, pl.ds(2 * HEAD_DIM, HEAD_DIM)], wsem.at[4]),
        pltpu.make_async_copy(wo_hbm, wod.at[pl.ds(0, HEAD_DIM)], wsem.at[5]),
        pltpu.make_async_copy(wd_hbm, wod.at[pl.ds(HEAD_DIM, ff)], wsem.at[6]),
    )
    for c in x_load(0):
        c.start()
    for c in w_loads:
        c.start()
    res_loads = [pltpu.make_async_copy(x_hbm.at[:, pl.ds(res_col[ab], cw)], xres.at[ab], ressem.at[ab]) for ab in (0, 1)]
    for c in res_loads:
        c.start()
    kbuf[...] = jnp.zeros_like(kbuf)
    vbuf[...] = jnp.zeros_like(vbuf)

    def pair_copy(b):
        col = pl.multiple_of((1 - core) * half, half)
        return pltpu.make_async_remote_copy(
            src_ref=part.at[lax.rem(b, SLOTS), :, pl.ds(col, half)], dst_ref=quart.at[b],
            send_sem=pair_send.at[lax.rem(b, SLOTS)], recv_sem=pair_recv.at[b],
            device_id=dev(partner), device_id_type=pl.DeviceIdType.MESH)

    def hop(src, dst, st, b, ab, d, axis):
        return pltpu.make_async_remote_copy(
            src_ref=src, dst_ref=dst, send_sem=ssem.at[st, ab, d, lax.rem(b, 2)], recv_sem=rsem.at[st, ab, d, b],
            device_id=dev(near[axis][d]), device_id_type=pl.DeviceIdType.MESH)

    def qcols(ab, chunk, h=None):
        base = ab * quarter + wrap(chunk) * cw
        if h is None:
            return pl.ds(pl.multiple_of(base, cw), cw)
        return pl.ds(pl.multiple_of(base + h * ch, ch), ch)

    def ycols(ab, chunk, h=None):
        base = mine0 + ab * quarter + wrap(chunk) * cw
        if h is None:
            return pl.ds(pl.multiple_of(base, cw), cw)
        return pl.ds(pl.multiple_of(base + h * ch, ch), ch)

    def brows(chunk):
        return pl.ds(pl.multiple_of(wrap(chunk) * rw, rw), rw)

    def yrows(b, chunk=None):
        if chunk is None:
            return pl.ds(pl.multiple_of(b * ROWS, ROWS), ROWS)
        return pl.ds(pl.multiple_of(b * ROWS + wrap(chunk) * rw, rw), rw)

    def send1(b, ab, d):
        p = pos[ab]
        return hop(quart.at[b, :, qcols(ab, p + 2, d)], r1.at[lax.rem(b, RING), ab, d], 0, b, ab, d, ab)

    def send2(b, ab, d):
        p = pos[ab]
        return hop(quart.at[b, :, qcols(ab, p + 1 - 2 * d)], r2.at[lax.rem(b, RING), ab, d], 1, b, ab, d, ab)

    def send3(b, ab, d):
        p2 = pos[1 - ab]
        return hop(quart.at[b, brows(p2 + 2), qcols(ab, pos[ab], d)], r3.at[b, ab, d], 2, b, ab, d, 1 - ab)

    def send4(b, ab, d):
        p2 = pos[1 - ab]
        return hop(quart.at[b, brows(p2 + 1 - 2 * d), qcols(ab, pos[ab])], r4.at[b, ab, d], 3, b, ab, d, 1 - ab)

    def y_hop(b, rows, cols, st, ab, d, axis):
        return hop(ybuf.at[rows, cols], ybuf.at[rows, cols], st, b, ab, d, axis)

    def send5(b, ab, d):
        return y_hop(b, yrows(b, pos[1 - ab]), ycols(ab, pos[ab]), 4, ab, d, 1 - ab)

    def land5(b, ab, d):
        return y_hop(b, yrows(b, pos[1 - ab] - 1 + 2 * d), ycols(ab, pos[ab]), 4, ab, d, 1 - ab)

    def send6(b, ab, d):
        return y_hop(b, yrows(b, pos[1 - ab] - 1 + 2 * d), ycols(ab, pos[ab], d), 5, ab, d, 1 - ab)

    def land6(b, ab, d):
        return y_hop(b, yrows(b, pos[1 - ab] + 2), ycols(ab, pos[ab], d), 5, ab, d, 1 - ab)

    def send7(b, ab, d):
        return y_hop(b, yrows(b), ycols(ab, pos[ab]), 6, ab, d, ab)

    def land7(b, ab, d):
        return y_hop(b, yrows(b), ycols(ab, pos[ab] - 1 + 2 * d), 6, ab, d, ab)

    def send8(b, ab, d):
        return y_hop(b, yrows(b), ycols(ab, pos[ab] - 1 + 2 * d, d), 7, ab, d, ab)

    def land8(b, ab, d):
        return y_hop(b, yrows(b), ycols(ab, pos[ab] + 2, d), 7, ab, d, ab)

    sends = (send1, send2, send3, send4, send5, send6, send7, send8)

    def gpair(b, c):
        cols = pl.ds(pl.multiple_of(c * half, half), half)
        return pltpu.make_async_remote_copy(
            src_ref=ybuf.at[yrows(b), cols], dst_ref=ybuf.at[yrows(b), cols],
            send_sem=gpair_send.at[lax.rem(b, 2)], recv_sem=gpair_recv.at[b],
            device_id=dev(partner), device_id_type=pl.DeviceIdType.MESH)

    def wait_all(copies):
        for cp in copies:
            cp.wait()

    def kv_store(b):
        rows = yrows(b)
        slot = lax.rem(b, 2)
        return (pltpu.make_async_copy(kbuf.at[rows], k_hbm.at[rows], kvsem.at[slot, 0]),
                pltpu.make_async_copy(vbuf.at[rows], v_hbm.at[rows], kvsem.at[slot, 1]))

    def issue(send, b):
        @pl.when(b >= 2)
        def _():
            both(lambda ab, d: send(b - 2, ab, d).wait_send())

        both(lambda ab, d: send(b, ab, d).start())

    def attend(q, b, keys):
        s = lax.dot_general(q, kbuf[pl.ds(0, keys), :], (((1,), (1,)), ((), ())), preferred_element_type=F32)
        edge = keys - KEYS
        tail = s[:, edge:]
        qpos = b * ROWS + lax.broadcasted_iota(jnp.int32, tail.shape, 0)
        kpos = edge + lax.broadcasted_iota(jnp.int32, tail.shape, 1)
        tail = jnp.where(kpos <= qpos, tail, -1e30)
        s = jnp.concatenate([s[:, :edge], tail], axis=1) if edge else tail
        top = jnp.max(s, axis=-1, keepdims=True)
        e = jnp.exp2((s - top) * (math.log2(math.e) / math.sqrt(HEAD_DIM)))
        probs = (e * (1.0 / jnp.sum(e, axis=-1, keepdims=True))).astype(BF16)
        o = jnp.dot(probs, vbuf[pl.ds(0, keys), :], preferred_element_type=F32)
        ombuf[:, pl.ds(0, HEAD_DIM)] = o.astype(BF16)

    def norm_rows(r):
        rows = pl.ds(r, 16)
        sums = [jnp.zeros((16, LANES), F32)] * 2
        for j in range(width // LANES):
            xr = xbuf[rows, pl.ds(j * LANES, LANES)].astype(F32)
            sums[j % 2] = sums[j % 2] + xr * xr
        mean = jnp.sum(sums[0] + sums[1], axis=-1, keepdims=True) * (1.0 / width)
        inv = jnp.broadcast_to(lax.rsqrt(mean + NORM_EPS), (16, LANES))
        for j in range(width // LANES):
            cols = pl.ds(j * LANES, LANES)
            abuf[rows, cols] = (xbuf[rows, cols].astype(F32) * inv * gbuf[:, cols]).astype(BF16)

    def prepare():
        for j in range(width // LANES):
            gbuf[:, j * LANES:(j + 1) * LANES] = jnp.broadcast_to(g_ref[j:j + 1, :].astype(F32), (16, LANES))
        wait_all(x_load(0))

        @pl.loop(0, ROWS // 16)
        def _(i):
            norm_rows(pl.multiple_of(i * 16, 16))

        for cp in x_load(1):
            cp.start()

        wait_all(w_loads[:2])

        @pl.loop(0, width // KEYS)
        def _(i):
            rows = pl.ds(pl.multiple_of(i * KEYS, KEYS), KEYS)
            for m in range(0, 2 * ff, LANES):
                wall[rows, pl.ds(3 * HEAD_DIM + m, LANES)] = wgu[pl.ds(m, LANES), rows].T

        wait_all(w_loads[2:5])

    tiles = width // OUT_TILE

    def compute(b):
        slot = lax.rem(b, 2)
        proj = jnp.dot(abuf[...], wall[...], preferred_element_type=F32)
        cos_t = tabs[slot, 0]
        sin_t = tabs[slot, 1]

        def rope(z):
            return (z * cos_t + pltpu.roll(z, HEAD_DIM // 2, 1) * sin_t).astype(BF16)

        q = rope(proj[:, :HEAD_DIM])
        rows = yrows(b)
        kbuf[rows, :] = rope(proj[:, HEAD_DIM:2 * HEAD_DIM])
        vbuf[rows, :] = proj[:, 2 * HEAD_DIM:3 * HEAD_DIM].astype(BF16)
        gate = proj[:, 3 * HEAD_DIM:3 * HEAD_DIM + ff]
        up = proj[:, 3 * HEAD_DIM + ff:]
        ombuf[:, pl.ds(HEAD_DIM, ff)] = (gate * jax.nn.sigmoid(gate) * up).astype(BF16)

        @pl.when(b >= 2)
        def _():
            wait_all(kv_store(b - 2))

        for cp in kv_store(b):
            cp.start()

        for n in range(tokens // KEYS):
            @pl.when(b * ROWS // KEYS == n)
            def _(n=n):
                attend(q, b, (n + 1) * KEYS)

        @pl.when(b == 0)
        def _():
            wait_all(w_loads[5:])

        @pl.when(b >= SLOTS)
        def _():
            pair_copy(b - SLOTS).wait_send()

        @pl.when(b + 1 < nblk)
        def _():
            wait_all(x_load(b + 1))

        om = ombuf[...]
        for n in range(tiles):
            cols = pl.ds(n * OUT_TILE, OUT_TILE)
            part[slot, :, cols] = jnp.dot(om, wod[:, cols], preferred_element_type=F32).astype(BF16)
            for r in range(n * ROWS // tiles, (n + 1) * ROWS // tiles, 16):
                norm_rows(r)
        pair_copy(b).start()

        @pl.when(b + 2 < nblk)
        def _():
            for cp in x_load(b + 2):
                cp.start()

    def add(dst, *srcs):
        total = dst[...].astype(F32)
        for s in srcs:
            total = total + s[...].astype(F32)
        dst[...] = total.astype(BF16)

    def both(f):
        for ab in (0, 1):
            for d in (0, 1):
                f(ab, d)

    def stage1(b):
        pair_copy(b).wait_recv()
        mine = pl.ds(pl.multiple_of(mine0, half), half)
        for r in range(0, ROWS, 32):
            add(quart.at[b, pl.ds(r, 32), :], part.at[lax.rem(b, SLOTS), pl.ds(r, 32), mine])
        issue(send1, b)

    def stage2(b):
        both(lambda ab, d: send1(b, ab, d).wait_recv())
        both(lambda ab, d: add(quart.at[b, :, qcols(ab, pos[ab] + 1 - 2 * d, d)], r1.at[lax.rem(b, RING), ab, d]))
        issue(send2, b)

    def stage3(b):
        both(lambda ab, d: send2(b, ab, d).wait_recv())
        for ab in (0, 1):
            add(quart.at[b, :, qcols(ab, pos[ab])], r2.at[lax.rem(b, RING), ab, 0], r2.at[lax.rem(b, RING), ab, 1])
        issue(send3, b)

    def stage4(b):
        both(lambda ab, d: send3(b, ab, d).wait_recv())
        both(lambda ab, d: add(quart.at[b, brows(pos[1 - ab] + 1 - 2 * d), qcols(ab, pos[ab], d)], r3.at[b, ab, d]))
        issue(send4, b)

    def stage5(b):
        @pl.when(b == 0)
        def _():
            for c in res_loads:
                c.wait()

        both(lambda ab, d: send4(b, ab, d).wait_recv())
        for ab in (0, 1):
            p2 = pos[1 - ab]
            total = quart[b, brows(p2), qcols(ab, pos[ab])].astype(F32)
            total = total + r4[b, ab, 0].astype(F32) + r4[b, ab, 1].astype(F32)
            total = total + xres[ab, yrows(b, p2), :].astype(F32)
            ybuf[yrows(b, p2), ycols(ab, pos[ab])] = total.astype(BF16)
        issue(send5, b)

    def stage6(b):
        both(lambda ab, d: land5(b, ab, d).wait_recv())
        issue(send6, b)

    def stage7(b):
        both(lambda ab, d: land6(b, ab, d).wait_recv())
        issue(send7, b)

    def stage8(b):
        both(lambda ab, d: land7(b, ab, d).wait_recv())
        issue(send8, b)

    def stage9(b):
        both(lambda ab, d: land8(b, ab, d).wait_recv())

        @pl.when(b >= 2)
        def _():
            gpair(b - 2, core).wait_send()

        gpair(b, core).start()

    def stage10(b):
        gpair(b, 1 - core).wait_recv()

    stages = (stage1, stage2, stage3, stage4, stage5, stage6, stage7, stage8, stage9, stage10)

    prepare()
    pl.semaphore_wait(barrier, 5)

    @pl.loop(0, nblk + LAG[-1])
    def _(t):
        @pl.when(t < nblk)
        def _():
            compute(t)

        for lag, stage in zip(LAG, stages):
            b = t - lag

            @pl.when((b >= 0) & (b < nblk))
            def _(b=b, stage=stage):
                stage(b)

    for b in range(nblk - SLOTS, nblk):
        pair_copy(b).wait_send()
    for b in range(nblk - 2, nblk):
        for send in sends:
            both(lambda ab, d: send(b, ab, d).wait_send())
        gpair(b, core).wait_send()
    for b in range(nblk - 2, nblk):
        wait_all(kv_store(b))


def rope_tables(tokens):
    inv_freq = np.float32(ROPE_BASE) ** (-np.arange(0, HEAD_DIM, 2, dtype=np.float32) / np.float32(HEAD_DIM))
    angles = np.arange(tokens, dtype=np.float32)[:, None] * inv_freq[None, :]
    cos_half, sin_half = np.cos(angles), np.sin(angles)
    return np.stack([np.concatenate([cos_half, cos_half], axis=1), np.concatenate([-sin_half, sin_half], axis=1)])


def solution(mesh):
    tp_size = mesh.shape['tp']
    side = math.isqrt(tp_size // 2)

    def local_layer(x_in, g_norm, w_q, w_k, w_v, w_o, w_gate, w_up, w_down):
        tokens, width = x_in.shape
        kv_heads = w_k.shape[1] // HEAD_DIM
        ff = w_gate.shape[1]
        nblk = tokens // ROWS
        half = width // 2
        cw = half // 2 // side
        rw = ROWS // side
        any_spec = pl.BlockSpec(memory_space=pl.ANY)
        y, k, v = pl.pallas_call(
            functools.partial(layer_kernel, (tp_size, side, kv_heads)),
            out_shape=(pltpu.VMEM((tokens, width), BF16),
                       jax.ShapeDtypeStruct((tokens, HEAD_DIM), BF16),
                       jax.ShapeDtypeStruct((tokens, HEAD_DIM), BF16)),
            in_specs=[any_spec, pl.BlockSpec(memory_space=pltpu.VMEM)] + [any_spec] * 8,
            out_specs=(pl.BlockSpec(memory_space=pltpu.VMEM), any_spec, any_spec),
            scratch_shapes=[
                pltpu.VMEM((width, 3 * HEAD_DIM + 2 * ff), BF16),
                pltpu.VMEM((2 * ff, width), BF16),
                pltpu.VMEM((HEAD_DIM + ff, width), BF16),
                pltpu.VMEM((ROWS, width), BF16),
                pltpu.VMEM((2, 2, ROWS, HEAD_DIM), F32),
                pltpu.VMEM((ROWS, width), BF16),
                pltpu.VMEM((16, width), F32),
                pltpu.VMEM((ROWS, HEAD_DIM + ff), BF16),
                pltpu.VMEM((tokens, HEAD_DIM), BF16),
                pltpu.VMEM((tokens, HEAD_DIM), BF16),
                pltpu.VMEM((SLOTS, ROWS, width), BF16),
                pltpu.VMEM((nblk, ROWS, half), BF16),
                pltpu.VMEM((RING, 2, 2, ROWS, cw // 2), BF16),
                pltpu.VMEM((RING, 2, 2, ROWS, cw), BF16),
                pltpu.VMEM((nblk, 2, 2, rw, cw // 2), BF16),
                pltpu.VMEM((nblk, 2, 2, rw, cw), BF16),
                pltpu.VMEM((2, tokens, cw), BF16),
                pltpu.SemaphoreType.DMA((7,)),
                pltpu.SemaphoreType.DMA((2, 2)),
                pltpu.SemaphoreType.DMA((2,)),
                pltpu.SemaphoreType.DMA((2, 2)),
                pltpu.SemaphoreType.DMA((SLOTS,)),
                pltpu.SemaphoreType.DMA((nblk,)),
                pltpu.SemaphoreType.DMA((8, 2, 2, 2)),
                pltpu.SemaphoreType.DMA((8, 2, 2, nblk)),
                pltpu.SemaphoreType.DMA((2,)),
                pltpu.SemaphoreType.DMA((nblk,)),
            ],
            compiler_params=pltpu.CompilerParams(collective_id=0, has_side_effects=True, vmem_limit_bytes=47 * 1024 * 1024),
            name="layer",
        )(x_in, g_norm.reshape(width // LANES, LANES), jnp.asarray(rope_tables(tokens)), w_q, w_k, w_v, w_o, w_gate.T, w_up.T, w_down)
        return y, k.reshape(tokens, 1, HEAD_DIM), v.reshape(tokens, 1, HEAD_DIM)

    return jax.shard_map(local_layer, mesh=mesh, in_specs=(P('dp', None), P(None), P(None, 'tp'), P(None, None), P(None, None), P('tp', None), P(None, 'tp'), P(None, 'tp'), P('tp', None)), out_specs=(P('dp', None), P('dp', 'tp', None), P('dp', 'tp', None)), check_vma=False)
```

```python
import functools
import math
import jax
import jax.numpy as jnp
import numpy as np
from jax import lax
from jax.experimental import pallas as pl
from jax.experimental.pallas import tpu as pltpu
from jax.sharding import PartitionSpec as P

HEAD_DIM = 128
ROPE_BASE = 500000.0
NORM_EPS = 1e-5
LANES = 128
ROWS = 128
SLOTS = 2
RING = 4
KEYS = 512
OUT_TILE = 512
LAG = (1, 2, 3, 4, 5, 6, 7, 8, 9, 10)
FIRST = (1, 2, 3, 4, 5)
SECOND = (6, 7, 8, 9, 10)
BF16 = jnp.bfloat16
F32 = jnp.float32


def layer_kernel(cfg, x_hbm, g_ref, tab_hbm, wq_hbm, wk_hbm, wv_hbm, wo_hbm, wg_hbm, wu_hbm, wd_hbm,
                 ybuf, kbuf, vbuf,
                 wall, wgu, wod, xbuf, tabs, abuf, gbuf, ombuf, part, quart, r1, r2, r3, r4, xres,
                 wsem, xsem, ressem, pair_send, pair_recv, ssem, rsem, gpair_send, gpair_recv):
    tokens, width = x_hbm.shape
    tp, side, kv_heads = cfg[:3]
    nblk = tokens // ROWS
    half = width // 2
    quarter = half // 2
    cw = quarter // side
    ch = cw // 2
    rw = ROWS // side
    ff = wg_hbm.shape[0]

    me = lax.axis_index("tp")
    core = lax.rem(me, 2)
    px = lax.rem(me // 2, side)
    py = me // (2 * side)
    partner = me + 1 - 2 * core

    def wrap(p):
        return lax.rem(p + side, side)

    def at(y, x):
        return (wrap(y) * side + wrap(x)) * 2 + core

    near = (((at(py, px + 1)), (at(py, px - 1))), ((at(py + 1, px)), (at(py - 1, px))))
    pos = (px, py)

    def dev(d):
        return {"tp": d}

    barrier = pltpu.get_barrier_semaphore()
    for d in (partner, *near[0], *near[1]):
        pl.semaphore_signal(barrier, inc=1, device_id=dev(d), device_id_type=pl.DeviceIdType.MESH)

    head = lax.div(me * kv_heads, tp)
    kcol = pl.ds(pl.multiple_of(head * HEAD_DIM, HEAD_DIM), HEAD_DIM)
    mine0 = core * half
    res_col = [pl.multiple_of(mine0 + ab * quarter + pos[ab] * cw, cw) for ab in (0, 1)]

    def x_load(b):
        rows = pl.ds(pl.multiple_of(b * ROWS, ROWS), ROWS)
        slot = lax.rem(b, 2)
        return (pltpu.make_async_copy(x_hbm.at[rows], xbuf, xsem.at[slot, 0]),
                pltpu.make_async_copy(tab_hbm.at[:, rows], tabs.at[slot], xsem.at[slot, 1]))

    w_loads = (
        pltpu.make_async_copy(wg_hbm, wgu.at[pl.ds(0, ff)], wsem.at[0]),
        pltpu.make_async_copy(wu_hbm, wgu.at[pl.ds(ff, ff)], wsem.at[1]),
        pltpu.make_async_copy(wq_hbm, wall.at[:, pl.ds(0, HEAD_DIM)], wsem.at[2]),
        pltpu.make_async_copy(wk_hbm.at[:, kcol], wall.at[:, pl.ds(HEAD_DIM, HEAD_DIM)], wsem.at[3]),
        pltpu.make_async_copy(wv_hbm.at[:, kcol], wall.at[:, pl.ds(2 * HEAD_DIM, HEAD_DIM)], wsem.at[4]),
        pltpu.make_async_copy(wo_hbm, wod.at[pl.ds(0, HEAD_DIM)], wsem.at[5]),
        pltpu.make_async_copy(wd_hbm, wod.at[pl.ds(HEAD_DIM, ff)], wsem.at[6]),
    )
    for c in x_load(0):
        c.start()
    for c in w_loads:
        c.start()
    res_loads = [pltpu.make_async_copy(x_hbm.at[:, pl.ds(res_col[ab], cw)], xres.at[ab], ressem.at[ab]) for ab in (0, 1)]
    for c in res_loads:
        c.start()
    kbuf[...] = jnp.zeros_like(kbuf)
    vbuf[...] = jnp.zeros_like(vbuf)

    def pair_copy(b):
        col = pl.multiple_of((1 - core) * half, half)
        return pltpu.make_async_remote_copy(
            src_ref=part.at[lax.rem(b, SLOTS), :, pl.ds(col, half)], dst_ref=quart.at[b],
            send_sem=pair_send.at[lax.rem(b, SLOTS)], recv_sem=pair_recv.at[b],
            device_id=dev(partner), device_id_type=pl.DeviceIdType.MESH)

    def hop(src, dst, st, b, ab, d, axis):
        return pltpu.make_async_remote_copy(
            src_ref=src, dst_ref=dst, send_sem=ssem.at[st, ab, d, lax.rem(b, 2)], recv_sem=rsem.at[st, ab, d, b],
            device_id=dev(near[axis][d]), device_id_type=pl.DeviceIdType.MESH)

    def qcols(ab, chunk, h=None):
        base = ab * quarter + wrap(chunk) * cw
        if h is None:
            return pl.ds(pl.multiple_of(base, cw), cw)
        return pl.ds(pl.multiple_of(base + h * ch, ch), ch)

    def ycols(ab, chunk, h=None):
        base = mine0 + ab * quarter + wrap(chunk) * cw
        if h is None:
            return pl.ds(pl.multiple_of(base, cw), cw)
        return pl.ds(pl.multiple_of(base + h * ch, ch), ch)

    def brows(chunk):
        return pl.ds(pl.multiple_of(wrap(chunk) * rw, rw), rw)

    def yrows(b, chunk=None):
        if chunk is None:
            return pl.ds(pl.multiple_of(b * ROWS, ROWS), ROWS)
        return pl.ds(pl.multiple_of(b * ROWS + wrap(chunk) * rw, rw), rw)

    def send1(b, ab, d):
        p = pos[ab]
        return hop(quart.at[b, :, qcols(ab, p + 2, d)], r1.at[lax.rem(b, RING), ab, d], 0, b, ab, d, ab)

    def send2(b, ab, d):
        p = pos[ab]
        return hop(quart.at[b, :, qcols(ab, p + 1 - 2 * d)], r2.at[lax.rem(b, RING), ab, d], 1, b, ab, d, ab)

    def send3(b, ab, d):
        p2 = pos[1 - ab]
        return hop(quart.at[b, brows(p2 + 2), qcols(ab, pos[ab], d)], r3.at[b, ab, d], 2, b, ab, d, 1 - ab)

    def send4(b, ab, d):
        p2 = pos[1 - ab]
        return hop(quart.at[b, brows(p2 + 1 - 2 * d), qcols(ab, pos[ab])], r4.at[b, ab, d], 3, b, ab, d, 1 - ab)

    def y_hop(b, rows, cols, st, ab, d, axis):
        return hop(ybuf.at[rows, cols], ybuf.at[rows, cols], st, b, ab, d, axis)

    def send5(b, ab, d):
        return y_hop(b, yrows(b, pos[1 - ab]), ycols(ab, pos[ab]), 4, ab, d, 1 - ab)

    def land5(b, ab, d):
        return y_hop(b, yrows(b, pos[1 - ab] - 1 + 2 * d), ycols(ab, pos[ab]), 4, ab, d, 1 - ab)

    def send6(b, ab, d):
        return y_hop(b, yrows(b, pos[1 - ab] - 1 + 2 * d), ycols(ab, pos[ab], d), 5, ab, d, 1 - ab)

    def land6(b, ab, d):
        return y_hop(b, yrows(b, pos[1 - ab] + 2), ycols(ab, pos[ab], d), 5, ab, d, 1 - ab)

    def send7(b, ab, d):
        return y_hop(b, yrows(b), ycols(ab, pos[ab]), 6, ab, d, ab)

    def land7(b, ab, d):
        return y_hop(b, yrows(b), ycols(ab, pos[ab] - 1 + 2 * d), 6, ab, d, ab)

    def send8(b, ab, d):
        return y_hop(b, yrows(b), ycols(ab, pos[ab] - 1 + 2 * d, d), 7, ab, d, ab)

    def land8(b, ab, d):
        return y_hop(b, yrows(b), ycols(ab, pos[ab] + 2, d), 7, ab, d, ab)

    sends = (send1, send2, send3, send4, send5, send6, send7, send8)

    def gpair(b, c):
        cols = pl.ds(pl.multiple_of(c * half, half), half)
        return pltpu.make_async_remote_copy(
            src_ref=ybuf.at[yrows(b), cols], dst_ref=ybuf.at[yrows(b), cols],
            send_sem=gpair_send.at[lax.rem(b, 2)], recv_sem=gpair_recv.at[b],
            device_id=dev(partner), device_id_type=pl.DeviceIdType.MESH)

    def wait_all(copies):
        for cp in copies:
            cp.wait()

    def issue(send, b):
        @pl.when(b >= 2)
        def _():
            both(lambda ab, d: send(b - 2, ab, d).wait_send())

        both(lambda ab, d: send(b, ab, d).start())

    def attend(q, b, keys):
        s = lax.dot_general(q, kbuf[pl.ds(0, keys), :], (((1,), (1,)), ((), ())), preferred_element_type=F32)
        edge = keys - KEYS
        tail = s[:, edge:]
        qpos = b * ROWS + lax.broadcasted_iota(jnp.int32, tail.shape, 0)
        kpos = edge + lax.broadcasted_iota(jnp.int32, tail.shape, 1)
        tail = jnp.where(kpos <= qpos, tail, -1e30)
        s = jnp.concatenate([s[:, :edge], tail], axis=1) if edge else tail
        top = jnp.max(s, axis=-1, keepdims=True)
        e = jnp.exp2((s - top) * (math.log2(math.e) / math.sqrt(HEAD_DIM)))
        probs = (e * (1.0 / jnp.sum(e, axis=-1, keepdims=True))).astype(BF16)
        o = jnp.dot(probs, vbuf[pl.ds(0, keys), :], preferred_element_type=F32)
        ombuf[:, pl.ds(0, HEAD_DIM)] = o.astype(BF16)

    def norm_rows(r):
        rows = pl.ds(r, 16)
        sums = [jnp.zeros((16, LANES), F32)] * 2
        for j in range(width // LANES):
            xr = xbuf[rows, pl.ds(j * LANES, LANES)].astype(F32)
            sums[j % 2] = sums[j % 2] + xr * xr
        mean = jnp.sum(sums[0] + sums[1], axis=-1, keepdims=True) * (1.0 / width)
        inv = jnp.broadcast_to(lax.rsqrt(mean + NORM_EPS), (16, LANES))
        for j in range(width // LANES):
            cols = pl.ds(j * LANES, LANES)
            abuf[rows, cols] = (xbuf[rows, cols].astype(F32) * inv * gbuf[:, cols]).astype(BF16)

    def prepare():
        for j in range(width // LANES):
            gbuf[:, j * LANES:(j + 1) * LANES] = jnp.broadcast_to(g_ref[j:j + 1, :].astype(F32), (16, LANES))
        wait_all(x_load(0))

        @pl.loop(0, ROWS // 16)
        def _(i):
            norm_rows(pl.multiple_of(i * 16, 16))

        for cp in x_load(1):
            cp.start()

        wait_all(w_loads[:2])

        @pl.loop(0, width // KEYS)
        def _(i):
            rows = pl.ds(pl.multiple_of(i * KEYS, KEYS), KEYS)
            for m in range(0, 2 * ff, LANES):
                wall[rows, pl.ds(3 * HEAD_DIM + m, LANES)] = wgu[pl.ds(m, LANES), rows].T

        wait_all(w_loads[2:5])

    tiles = width // OUT_TILE

    def compute(b):
        slot = lax.rem(b, 2)
        proj = jnp.dot(abuf[...], wall[...], preferred_element_type=F32)
        cos_t = tabs[slot, 0]
        sin_t = tabs[slot, 1]

        def rope(z):
            return (z * cos_t + pltpu.roll(z, HEAD_DIM // 2, 1) * sin_t).astype(BF16)

        q = rope(proj[:, :HEAD_DIM])
        rows = yrows(b)
        kbuf[rows, :] = rope(proj[:, HEAD_DIM:2 * HEAD_DIM])
        vbuf[rows, :] = proj[:, 2 * HEAD_DIM:3 * HEAD_DIM].astype(BF16)
        gate = proj[:, 3 * HEAD_DIM:3 * HEAD_DIM + ff]
        up = proj[:, 3 * HEAD_DIM + ff:]
        ombuf[:, pl.ds(HEAD_DIM, ff)] = (gate * jax.nn.sigmoid(gate) * up).astype(BF16)

        for n in range(tokens // KEYS):
            @pl.when(b * ROWS // KEYS == n)
            def _(n=n):
                attend(q, b, (n + 1) * KEYS)

    def finish(b):
        slot = lax.rem(b, 2)

        @pl.when(b == 0)
        def _():
            wait_all(w_loads[5:])

        @pl.when(b >= SLOTS)
        def _():
            pair_copy(b - SLOTS).wait_send()

        @pl.when(b + 1 < nblk)
        def _():
            wait_all(x_load(b + 1))

        om = ombuf[...]
        for n in range(tiles):
            cols = pl.ds(n * OUT_TILE, OUT_TILE)
            part[slot, :, cols] = jnp.dot(om, wod[:, cols], preferred_element_type=F32).astype(BF16)
            for r in range(n * ROWS // tiles, (n + 1) * ROWS // tiles, 16):
                norm_rows(r)
        pair_copy(b).start()

        @pl.when(b + 2 < nblk)
        def _():
            for cp in x_load(b + 2):
                cp.start()

    def add(dst, *srcs):
        total = dst[...].astype(F32)
        for s in srcs:
            total = total + s[...].astype(F32)
        dst[...] = total.astype(BF16)

    def both(f):
        for ab in (0, 1):
            for d in (0, 1):
                f(ab, d)

    def stage1(b):
        pair_copy(b).wait_recv()
        mine = pl.ds(pl.multiple_of(mine0, half), half)
        for r in range(0, ROWS, 32):
            add(quart.at[b, pl.ds(r, 32), :], part.at[lax.rem(b, SLOTS), pl.ds(r, 32), mine])
        issue(send1, b)

    def stage2(b):
        both(lambda ab, d: send1(b, ab, d).wait_recv())
        both(lambda ab, d: add(quart.at[b, :, qcols(ab, pos[ab] + 1 - 2 * d, d)], r1.at[lax.rem(b, RING), ab, d]))
        issue(send2, b)

    def stage3(b):
        both(lambda ab, d: send2(b, ab, d).wait_recv())
        for ab in (0, 1):
            add(quart.at[b, :, qcols(ab, pos[ab])], r2.at[lax.rem(b, RING), ab, 0], r2.at[lax.rem(b, RING), ab, 1])
        issue(send3, b)

    def stage4(b):
        both(lambda ab, d: send3(b, ab, d).wait_recv())
        both(lambda ab, d: add(quart.at[b, brows(pos[1 - ab] + 1 - 2 * d), qcols(ab, pos[ab], d)], r3.at[b, ab, d]))
        issue(send4, b)

    def stage5(b):
        @pl.when(b == 0)
        def _():
            for c in res_loads:
                c.wait()

        both(lambda ab, d: send4(b, ab, d).wait_recv())
        for ab in (0, 1):
            p2 = pos[1 - ab]
            total = quart[b, brows(p2), qcols(ab, pos[ab])].astype(F32)
            total = total + r4[b, ab, 0].astype(F32) + r4[b, ab, 1].astype(F32)
            total = total + xres[ab, yrows(b, p2), :].astype(F32)
            ybuf[yrows(b, p2), ycols(ab, pos[ab])] = total.astype(BF16)
        issue(send5, b)

    def stage6(b):
        both(lambda ab, d: land5(b, ab, d).wait_recv())
        issue(send6, b)

    def stage7(b):
        both(lambda ab, d: land6(b, ab, d).wait_recv())
        issue(send7, b)

    def stage8(b):
        both(lambda ab, d: land7(b, ab, d).wait_recv())
        issue(send8, b)

    def stage9(b):
        both(lambda ab, d: land8(b, ab, d).wait_recv())

        @pl.when(b >= 2)
        def _():
            gpair(b - 2, core).wait_send()

        gpair(b, core).start()

    def stage10(b):
        gpair(b, 1 - core).wait_recv()

    stages = (stage1, stage2, stage3, stage4, stage5, stage6, stage7, stage8, stage9, stage10)

    prepare()
    pl.semaphore_wait(barrier, 5)

    @pl.loop(0, nblk + LAG[-1])
    def _(t):
        def run(group):
            for n in group:
                b = t - LAG[n - 1]

                @pl.when((b >= 0) & (b < nblk))
                def _(b=b, n=n):
                    stages[n - 1](b)

        @pl.when(t < nblk)
        def _():
            compute(t)

        run(FIRST)

        @pl.when(t < nblk)
        def _():
            finish(t)

        run(SECOND)

    for b in range(nblk - SLOTS, nblk):
        pair_copy(b).wait_send()
    for b in range(nblk - 2, nblk):
        for send in sends:
            both(lambda ab, d: send(b, ab, d).wait_send())
        gpair(b, core).wait_send()


def store_kernel(y_ref, k_ref, v_ref, y_hbm, k_hbm, v_hbm, sems):
    pieces = sems.shape[0] - 2
    rows = y_ref.shape[0] // pieces
    copies = [pltpu.make_async_copy(y_ref.at[pl.ds(i * rows, rows)], y_hbm.at[pl.ds(i * rows, rows)], sems.at[i])
              for i in range(pieces)]
    copies.append(pltpu.make_async_copy(k_ref, k_hbm, sems.at[pieces]))
    copies.append(pltpu.make_async_copy(v_ref, v_hbm, sems.at[pieces + 1]))
    for cp in copies:
        cp.start()
    for cp in copies:
        cp.wait()


def rope_tables(tokens):
    inv_freq = np.float32(ROPE_BASE) ** (-np.arange(0, HEAD_DIM, 2, dtype=np.float32) / np.float32(HEAD_DIM))
    angles = np.arange(tokens, dtype=np.float32)[:, None] * inv_freq[None, :]
    cos_half, sin_half = np.cos(angles), np.sin(angles)
    return np.stack([np.concatenate([cos_half, cos_half], axis=1), np.concatenate([-sin_half, sin_half], axis=1)])


def solution(mesh):
    tp_size = mesh.shape['tp']
    side = math.isqrt(tp_size // 2)

    def local_layer(x_in, g_norm, w_q, w_k, w_v, w_o, w_gate, w_up, w_down):
        tokens, width = x_in.shape
        kv_heads = w_k.shape[1] // HEAD_DIM
        ff = w_gate.shape[1]
        nblk = tokens // ROWS
        half = width // 2
        cw = half // 2 // side
        rw = ROWS // side
        any_spec = pl.BlockSpec(memory_space=pl.ANY)
        y, k, v = pl.pallas_call(
            functools.partial(layer_kernel, (tp_size, side, kv_heads)),
            out_shape=(pltpu.VMEM((tokens, width), BF16),
                       pltpu.VMEM((tokens, HEAD_DIM), BF16),
                       pltpu.VMEM((tokens, HEAD_DIM), BF16)),
            in_specs=[any_spec, pl.BlockSpec(memory_space=pltpu.VMEM)] + [any_spec] * 8,
            out_specs=(pl.BlockSpec(memory_space=pltpu.VMEM),) * 3,
            scratch_shapes=[
                pltpu.VMEM((width, 3 * HEAD_DIM + 2 * ff), BF16),
                pltpu.VMEM((2 * ff, width), BF16),
                pltpu.VMEM((HEAD_DIM + ff, width), BF16),
                pltpu.VMEM((ROWS, width), BF16),
                pltpu.VMEM((2, 2, ROWS, HEAD_DIM), F32),
                pltpu.VMEM((ROWS, width), BF16),
                pltpu.VMEM((16, width), F32),
                pltpu.VMEM((ROWS, HEAD_DIM + ff), BF16),
                pltpu.VMEM((SLOTS, ROWS, width), BF16),
                pltpu.VMEM((nblk, ROWS, half), BF16),
                pltpu.VMEM((RING, 2, 2, ROWS, cw // 2), BF16),
                pltpu.VMEM((RING, 2, 2, ROWS, cw), BF16),
                pltpu.VMEM((nblk, 2, 2, rw, cw // 2), BF16),
                pltpu.VMEM((nblk, 2, 2, rw, cw), BF16),
                pltpu.VMEM((2, tokens, cw), BF16),
                pltpu.SemaphoreType.DMA((7,)),
                pltpu.SemaphoreType.DMA((2, 2)),
                pltpu.SemaphoreType.DMA((2,)),
                pltpu.SemaphoreType.DMA((SLOTS,)),
                pltpu.SemaphoreType.DMA((nblk,)),
                pltpu.SemaphoreType.DMA((8, 2, 2, 2)),
                pltpu.SemaphoreType.DMA((8, 2, 2, nblk)),
                pltpu.SemaphoreType.DMA((2,)),
                pltpu.SemaphoreType.DMA((nblk,)),
            ],
            compiler_params=pltpu.CompilerParams(collective_id=0, has_side_effects=True, vmem_limit_bytes=46 * 1024 * 1024),
            name="layer",
        )(x_in, g_norm.reshape(width // LANES, LANES), jnp.asarray(rope_tables(tokens)), w_q, w_k, w_v, w_o, w_gate.T, w_up.T, w_down)
        y, k, v = pl.pallas_call(
            store_kernel,
            out_shape=(jax.ShapeDtypeStruct((tokens, width), BF16),
                       jax.ShapeDtypeStruct((tokens, HEAD_DIM), BF16),
                       jax.ShapeDtypeStruct((tokens, HEAD_DIM), BF16)),
            in_specs=[any_spec] * 3,
            out_specs=(any_spec,) * 3,
            scratch_shapes=[pltpu.SemaphoreType.DMA((10,))],
            compiler_params=pltpu.CompilerParams(vmem_limit_bytes=1024 * 1024),
            name="store",
        )(y, k, v)
        return y, k.reshape(tokens, 1, HEAD_DIM), v.reshape(tokens, 1, HEAD_DIM)

    return jax.shard_map(local_layer, mesh=mesh, in_specs=(P('dp', None), P(None), P(None, 'tp'), P(None, None), P(None, None), P('tp', None), P(None, 'tp'), P(None, 'tp'), P('tp', None)), out_specs=(P('dp', None), P('dp', 'tp', None), P('dp', 'tp', None)), check_vma=False)
```

```python
import functools
import math
import jax
import jax.numpy as jnp
import numpy as np
from jax import lax
from jax.experimental import pallas as pl
from jax.experimental.pallas import tpu as pltpu
from jax.sharding import PartitionSpec as P

HEAD_DIM = 128
ROPE_BASE = 500000.0
NORM_EPS = 1e-5
LANES = 128
ROWS = 128
SLOTS = 2
RING = 4
KEYS = 512
OUT_TILE = 512
LAG = (1, 2, 3, 4, 5, 6, 7, 9, 11, 12)
FIRST = (1, 2, 3, 4, 5)
SECOND = (6, 7, 8, 9, 10)
BF16 = jnp.bfloat16
F32 = jnp.float32


def layer_kernel(cfg, x_hbm, g_ref, tab_hbm, wq_hbm, wk_hbm, wv_hbm, wo_hbm, wg_hbm, wu_hbm, wd_hbm,
                 ybuf, kbuf, vbuf,
                 wall, wgu, wod, xbuf, tabs, abuf, gbuf, ombuf, part, quart, r1, r2, r3, r4, xres,
                 wsem, xsem, ressem, pair_send, pair_recv, ssem, rsem, gpair_send, gpair_recv):
    tokens, width = x_hbm.shape
    tp, side, kv_heads = cfg[:3]
    nblk = tokens // ROWS
    half = width // 2
    quarter = half // 2
    cw = quarter // side
    ch = cw // 2
    rw = ROWS // side
    ff = wg_hbm.shape[0]

    me = lax.axis_index("tp")
    core = lax.rem(me, 2)
    px = lax.rem(me // 2, side)
    py = me // (2 * side)
    partner = me + 1 - 2 * core

    def wrap(p):
        return lax.rem(p + side, side)

    def at(y, x):
        return (wrap(y) * side + wrap(x)) * 2 + core

    near = (((at(py, px + 1)), (at(py, px - 1))), ((at(py + 1, px)), (at(py - 1, px))))
    pos = (px, py)

    def dev(d):
        return {"tp": d}

    barrier = pltpu.get_barrier_semaphore()
    for d in (partner, *near[0], *near[1]):
        pl.semaphore_signal(barrier, inc=1, device_id=dev(d), device_id_type=pl.DeviceIdType.MESH)

    head = lax.div(me * kv_heads, tp)
    kcol = pl.ds(pl.multiple_of(head * HEAD_DIM, HEAD_DIM), HEAD_DIM)
    mine0 = core * half
    res_col = [pl.multiple_of(mine0 + ab * quarter + pos[ab] * cw, cw) for ab in (0, 1)]

    def x_load(b):
        rows = pl.ds(pl.multiple_of(b * ROWS, ROWS), ROWS)
        slot = lax.rem(b, 2)
        return (pltpu.make_async_copy(x_hbm.at[rows], xbuf, xsem.at[slot, 0]),
                pltpu.make_async_copy(tab_hbm.at[:, rows], tabs.at[slot], xsem.at[slot, 1]))

    w_loads = (
        pltpu.make_async_copy(wg_hbm, wgu.at[pl.ds(0, ff)], wsem.at[0]),
        pltpu.make_async_copy(wu_hbm, wgu.at[pl.ds(ff, ff)], wsem.at[1]),
        pltpu.make_async_copy(wq_hbm, wall.at[:, pl.ds(0, HEAD_DIM)], wsem.at[2]),
        pltpu.make_async_copy(wk_hbm.at[:, kcol], wall.at[:, pl.ds(HEAD_DIM, HEAD_DIM)], wsem.at[3]),
        pltpu.make_async_copy(wv_hbm.at[:, kcol], wall.at[:, pl.ds(2 * HEAD_DIM, HEAD_DIM)], wsem.at[4]),
        pltpu.make_async_copy(wo_hbm, wod.at[pl.ds(0, HEAD_DIM)], wsem.at[5]),
        pltpu.make_async_copy(wd_hbm, wod.at[pl.ds(HEAD_DIM, ff)], wsem.at[6]),
    )
    for c in x_load(0):
        c.start()
    for c in w_loads:
        c.start()
    res_loads = [pltpu.make_async_copy(x_hbm.at[:, pl.ds(res_col[ab], cw)], xres.at[ab], ressem.at[ab]) for ab in (0, 1)]
    for c in res_loads:
        c.start()
    kbuf[...] = jnp.zeros_like(kbuf)
    vbuf[...] = jnp.zeros_like(vbuf)

    def pair_copy(b):
        col = pl.multiple_of((1 - core) * half, half)
        return pltpu.make_async_remote_copy(
            src_ref=part.at[lax.rem(b, SLOTS), :, pl.ds(col, half)], dst_ref=quart.at[b],
            send_sem=pair_send.at[lax.rem(b, SLOTS)], recv_sem=pair_recv.at[b],
            device_id=dev(partner), device_id_type=pl.DeviceIdType.MESH)

    def hop(src, dst, st, b, ab, d, axis):
        return pltpu.make_async_remote_copy(
            src_ref=src, dst_ref=dst, send_sem=ssem.at[st, ab, d, lax.rem(b, 2)], recv_sem=rsem.at[st, ab, d, b],
            device_id=dev(near[axis][d]), device_id_type=pl.DeviceIdType.MESH)

    def qcols(ab, chunk, h=None):
        base = ab * quarter + wrap(chunk) * cw
        if h is None:
            return pl.ds(pl.multiple_of(base, cw), cw)
        return pl.ds(pl.multiple_of(base + h * ch, ch), ch)

    def ycols(ab, chunk, h=None):
        base = mine0 + ab * quarter + wrap(chunk) * cw
        if h is None:
            return pl.ds(pl.multiple_of(base, cw), cw)
        return pl.ds(pl.multiple_of(base + h * ch, ch), ch)

    def brows(chunk):
        return pl.ds(pl.multiple_of(wrap(chunk) * rw, rw), rw)

    def yrows(b, chunk=None):
        if chunk is None:
            return pl.ds(pl.multiple_of(b * ROWS, ROWS), ROWS)
        return pl.ds(pl.multiple_of(b * ROWS + wrap(chunk) * rw, rw), rw)

    def send1(b, ab, d):
        p = pos[ab]
        return hop(quart.at[b, :, qcols(ab, p + 2, d)], r1.at[lax.rem(b, RING), ab, d], 0, b, ab, d, ab)

    def send2(b, ab, d):
        p = pos[ab]
        return hop(quart.at[b, :, qcols(ab, p + 1 - 2 * d)], r2.at[lax.rem(b, RING), ab, d], 1, b, ab, d, ab)

    def send3(b, ab, d):
        p2 = pos[1 - ab]
        return hop(quart.at[b, brows(p2 + 2), qcols(ab, pos[ab], d)], r3.at[b, ab, d], 2, b, ab, d, 1 - ab)

    def send4(b, ab, d):
        p2 = pos[1 - ab]
        return hop(quart.at[b, brows(p2 + 1 - 2 * d), qcols(ab, pos[ab])], r4.at[b, ab, d], 3, b, ab, d, 1 - ab)

    def y_hop(b, rows, cols, st, ab, d, axis):
        return hop(ybuf.at[rows, cols], ybuf.at[rows, cols], st, b, ab, d, axis)

    def send5(b, ab, d):
        return y_hop(b, yrows(b, pos[1 - ab]), ycols(ab, pos[ab]), 4, ab, d, 1 - ab)

    def land5(b, ab, d):
        return y_hop(b, yrows(b, pos[1 - ab] - 1 + 2 * d), ycols(ab, pos[ab]), 4, ab, d, 1 - ab)

    def send6(b, ab, d):
        return y_hop(b, yrows(b, pos[1 - ab] - 1 + 2 * d), ycols(ab, pos[ab], d), 5, ab, d, 1 - ab)

    def land6(b, ab, d):
        return y_hop(b, yrows(b, pos[1 - ab] + 2), ycols(ab, pos[ab], d), 5, ab, d, 1 - ab)

    def send7(b, ab, d):
        return y_hop(b, yrows(b), ycols(ab, pos[ab]), 6, ab, d, ab)

    def land7(b, ab, d):
        return y_hop(b, yrows(b), ycols(ab, pos[ab] - 1 + 2 * d), 6, ab, d, ab)

    def send8(b, ab, d):
        return y_hop(b, yrows(b), ycols(ab, pos[ab] - 1 + 2 * d, d), 7, ab, d, ab)

    def land8(b, ab, d):
        return y_hop(b, yrows(b), ycols(ab, pos[ab] + 2, d), 7, ab, d, ab)

    sends = (send1, send2, send3, send4, send5, send6, send7, send8)

    def gpair(b, c):
        cols = pl.ds(pl.multiple_of(c * half, half), half)
        return pltpu.make_async_remote_copy(
            src_ref=ybuf.at[yrows(b), cols], dst_ref=ybuf.at[yrows(b), cols],
            send_sem=gpair_send.at[lax.rem(b, 2)], recv_sem=gpair_recv.at[b],
            device_id=dev(partner), device_id_type=pl.DeviceIdType.MESH)

    def wait_all(copies):
        for cp in copies:
            cp.wait()

    def issue(send, b):
        @pl.when(b >= 2)
        def _():
            both(lambda ab, d: send(b - 2, ab, d).wait_send())

        both(lambda ab, d: send(b, ab, d).start())

    def attend(q, b, keys):
        s = lax.dot_general(q, kbuf[pl.ds(0, keys), :], (((1,), (1,)), ((), ())), preferred_element_type=F32)
        edge = keys - KEYS
        tail = s[:, edge:]
        qpos = b * ROWS + lax.broadcasted_iota(jnp.int32, tail.shape, 0)
        kpos = edge + lax.broadcasted_iota(jnp.int32, tail.shape, 1)
        tail = jnp.where(kpos <= qpos, tail, -1e30)
        s = jnp.concatenate([s[:, :edge], tail], axis=1) if edge else tail
        top = jnp.max(s, axis=-1, keepdims=True)
        e = jnp.exp2((s - top) * (math.log2(math.e) / math.sqrt(HEAD_DIM)))
        probs = (e * (1.0 / jnp.sum(e, axis=-1, keepdims=True))).astype(BF16)
        o = jnp.dot(probs, vbuf[pl.ds(0, keys), :], preferred_element_type=F32)
        ombuf[:, pl.ds(0, HEAD_DIM)] = o.astype(BF16)

    def norm_rows(r):
        rows = pl.ds(r, 16)
        sums = [jnp.zeros((16, LANES), F32)] * 2
        for j in range(width // LANES):
            xr = xbuf[rows, pl.ds(j * LANES, LANES)].astype(F32)
            sums[j % 2] = sums[j % 2] + xr * xr
        mean = jnp.sum(sums[0] + sums[1], axis=-1, keepdims=True) * (1.0 / width)
        inv = jnp.broadcast_to(lax.rsqrt(mean + NORM_EPS), (16, LANES))
        for j in range(width // LANES):
            cols = pl.ds(j * LANES, LANES)
            abuf[rows, cols] = (xbuf[rows, cols].astype(F32) * inv * gbuf[:, cols]).astype(BF16)

    def prepare():
        for j in range(width // LANES):
            gbuf[:, j * LANES:(j + 1) * LANES] = jnp.broadcast_to(g_ref[j:j + 1, :].astype(F32), (16, LANES))
        wait_all(x_load(0))

        @pl.loop(0, ROWS // 16)
        def _(i):
            norm_rows(pl.multiple_of(i * 16, 16))

        for cp in x_load(1):
            cp.start()

        split = ff // LANES * LANES
        for first, last, load in ((0, split, 0), (split, 2 * ff, 1)):
            wait_all(w_loads[load:load + 1])

            @pl.loop(0, width // KEYS)
            def _(i, first=first, last=last):
                rows = pl.ds(pl.multiple_of(i * KEYS, KEYS), KEYS)
                for m in range(first, last, LANES):
                    wall[rows, pl.ds(3 * HEAD_DIM + m, LANES)] = wgu[pl.ds(m, LANES), rows].T

        wait_all(w_loads[2:5])

    tiles = width // OUT_TILE

    def compute(b):
        slot = lax.rem(b, 2)
        proj = jnp.dot(abuf[...], wall[...], preferred_element_type=F32)
        cos_t = tabs[slot, 0]
        sin_t = tabs[slot, 1]

        def rope(z):
            return (z * cos_t + pltpu.roll(z, HEAD_DIM // 2, 1) * sin_t).astype(BF16)

        q = rope(proj[:, :HEAD_DIM])
        rows = yrows(b)
        kbuf[rows, :] = rope(proj[:, HEAD_DIM:2 * HEAD_DIM])
        vbuf[rows, :] = proj[:, 2 * HEAD_DIM:3 * HEAD_DIM].astype(BF16)
        gate = proj[:, 3 * HEAD_DIM:3 * HEAD_DIM + ff]
        up = proj[:, 3 * HEAD_DIM + ff:]
        ombuf[:, pl.ds(HEAD_DIM, ff)] = (gate * jax.nn.sigmoid(gate) * up).astype(BF16)

        for n in range(tokens // KEYS):
            @pl.when(b * ROWS // KEYS == n)
            def _(n=n):
                attend(q, b, (n + 1) * KEYS)

    def finish(b):
        slot = lax.rem(b, 2)

        @pl.when(b == 0)
        def _():
            wait_all(w_loads[5:])

        @pl.when(b >= SLOTS)
        def _():
            pair_copy(b - SLOTS).wait_send()

        @pl.when(b + 1 < nblk)
        def _():
            wait_all(x_load(b + 1))

        om = ombuf[...]
        for n in range(tiles):
            cols = pl.ds(n * OUT_TILE, OUT_TILE)
            for r in range(n * ROWS // tiles, (n + 1) * ROWS // tiles, 16):
                norm_rows(r)
            part[slot, :, cols] = jnp.dot(om, wod[:, cols], preferred_element_type=F32).astype(BF16)
        pair_copy(b).start()

        @pl.when(b + 2 < nblk)
        def _():
            for cp in x_load(b + 2):
                cp.start()

    def add(dst, *srcs):
        if len(srcs) == 1:
            dst[...] = dst[...] + srcs[0][...]
            return
        total = dst[...].astype(F32)
        for s in srcs:
            total = total + s[...].astype(F32)
        dst[...] = total.astype(BF16)

    def both(f):
        for ab in (0, 1):
            for d in (0, 1):
                f(ab, d)

    def stage1(b):
        pair_copy(b).wait_recv()
        mine = pl.ds(pl.multiple_of(mine0, half), half)
        for r in range(0, ROWS, 32):
            add(quart.at[b, pl.ds(r, 32), :], part.at[lax.rem(b, SLOTS), pl.ds(r, 32), mine])
        issue(send1, b)

    def stage2(b):
        both(lambda ab, d: send1(b, ab, d).wait_recv())
        both(lambda ab, d: add(quart.at[b, :, qcols(ab, pos[ab] + 1 - 2 * d, d)], r1.at[lax.rem(b, RING), ab, d]))
        issue(send2, b)

    def stage3(b):
        both(lambda ab, d: send2(b, ab, d).wait_recv())
        for ab in (0, 1):
            add(quart.at[b, :, qcols(ab, pos[ab])], r2.at[lax.rem(b, RING), ab, 0], r2.at[lax.rem(b, RING), ab, 1])
        issue(send3, b)

    def stage4(b):
        both(lambda ab, d: send3(b, ab, d).wait_recv())
        both(lambda ab, d: add(quart.at[b, brows(pos[1 - ab] + 1 - 2 * d), qcols(ab, pos[ab], d)], r3.at[b, ab, d]))
        issue(send4, b)

    def stage5(b):
        @pl.when(b == 0)
        def _():
            for c in res_loads:
                c.wait()

        both(lambda ab, d: send4(b, ab, d).wait_recv())
        for ab in (0, 1):
            p2 = pos[1 - ab]
            total = quart[b, brows(p2), qcols(ab, pos[ab])].astype(F32)
            total = total + r4[b, ab, 0].astype(F32) + r4[b, ab, 1].astype(F32)
            total = total + xres[ab, yrows(b, p2), :].astype(F32)
            ybuf[yrows(b, p2), ycols(ab, pos[ab])] = total.astype(BF16)
        issue(send5, b)

    def stage6(b):
        both(lambda ab, d: land5(b, ab, d).wait_recv())
        issue(send6, b)

    def stage7(b):
        both(lambda ab, d: land6(b, ab, d).wait_recv())
        issue(send7, b)

    def stage8(b):
        both(lambda ab, d: land7(b, ab, d).wait_recv())
        issue(send8, b)

    def stage9(b):
        both(lambda ab, d: land8(b, ab, d).wait_recv())

        @pl.when(b >= 2)
        def _():
            gpair(b - 2, core).wait_send()

        gpair(b, core).start()

    def stage10(b):
        gpair(b, 1 - core).wait_recv()

    stages = (stage1, stage2, stage3, stage4, stage5, stage6, stage7, stage8, stage9, stage10)

    prepare()
    pl.semaphore_wait(barrier, 5)

    @pl.loop(0, nblk + LAG[-1])
    def _(t):
        def run(group):
            for n in group:
                b = t - LAG[n - 1]

                @pl.when((b >= 0) & (b < nblk))
                def _(b=b, n=n):
                    stages[n - 1](b)

        @pl.when(t < nblk)
        def _():
            compute(t)

        run(FIRST)

        @pl.when(t < nblk)
        def _():
            finish(t)

        run(SECOND)

    for b in range(nblk - SLOTS, nblk):
        pair_copy(b).wait_send()
    for b in range(nblk - 2, nblk):
        for send in sends:
            both(lambda ab, d: send(b, ab, d).wait_send())
        gpair(b, core).wait_send()


def store_kernel(y_ref, k_ref, v_ref, y_hbm, k_hbm, v_hbm, sems):
    pieces = sems.shape[0] - 2
    rows = y_ref.shape[0] // pieces
    copies = [pltpu.make_async_copy(y_ref.at[pl.ds(i * rows, rows)], y_hbm.at[pl.ds(i * rows, rows)], sems.at[i])
              for i in range(pieces)]
    copies.append(pltpu.make_async_copy(k_ref, k_hbm, sems.at[pieces]))
    copies.append(pltpu.make_async_copy(v_ref, v_hbm, sems.at[pieces + 1]))
    for cp in copies:
        cp.start()
    for cp in copies:
        cp.wait()


def rope_tables(tokens):
    inv_freq = np.float32(ROPE_BASE) ** (-np.arange(0, HEAD_DIM, 2, dtype=np.float32) / np.float32(HEAD_DIM))
    angles = np.arange(tokens, dtype=np.float32)[:, None] * inv_freq[None, :]
    cos_half, sin_half = np.cos(angles), np.sin(angles)
    return np.stack([np.concatenate([cos_half, cos_half], axis=1), np.concatenate([-sin_half, sin_half], axis=1)])


def solution(mesh):
    tp_size = mesh.shape['tp']
    side = math.isqrt(tp_size // 2)

    def local_layer(x_in, g_norm, w_q, w_k, w_v, w_o, w_gate, w_up, w_down):
        tokens, width = x_in.shape
        kv_heads = w_k.shape[1] // HEAD_DIM
        ff = w_gate.shape[1]
        nblk = tokens // ROWS
        half = width // 2
        cw = half // 2 // side
        rw = ROWS // side
        any_spec = pl.BlockSpec(memory_space=pl.ANY)
        y, k, v = pl.pallas_call(
            functools.partial(layer_kernel, (tp_size, side, kv_heads)),
            out_shape=(pltpu.VMEM((tokens, width), BF16),
                       pltpu.VMEM((tokens, HEAD_DIM), BF16),
                       pltpu.VMEM((tokens, HEAD_DIM), BF16)),
            in_specs=[any_spec, pl.BlockSpec(memory_space=pltpu.VMEM)] + [any_spec] * 8,
            out_specs=(pl.BlockSpec(memory_space=pltpu.VMEM),) * 3,
            scratch_shapes=[
                pltpu.VMEM((width, 3 * HEAD_DIM + 2 * ff), BF16),
                pltpu.VMEM((2 * ff, width), BF16),
                pltpu.VMEM((HEAD_DIM + ff, width), BF16),
                pltpu.VMEM((ROWS, width), BF16),
                pltpu.VMEM((2, 2, ROWS, HEAD_DIM), F32),
                pltpu.VMEM((ROWS, width), BF16),
                pltpu.VMEM((16, width), F32),
                pltpu.VMEM((ROWS, HEAD_DIM + ff), BF16),
                pltpu.VMEM((SLOTS, ROWS, width), BF16),
                pltpu.VMEM((nblk, ROWS, half), BF16),
                pltpu.VMEM((RING, 2, 2, ROWS, cw // 2), BF16),
                pltpu.VMEM((RING, 2, 2, ROWS, cw), BF16),
                pltpu.VMEM((nblk, 2, 2, rw, cw // 2), BF16),
                pltpu.VMEM((nblk, 2, 2, rw, cw), BF16),
                pltpu.VMEM((2, tokens, cw), BF16),
                pltpu.SemaphoreType.DMA((7,)),
                pltpu.SemaphoreType.DMA((2, 2)),
                pltpu.SemaphoreType.DMA((2,)),
                pltpu.SemaphoreType.DMA((SLOTS,)),
                pltpu.SemaphoreType.DMA((nblk,)),
                pltpu.SemaphoreType.DMA((8, 2, 2, 2)),
                pltpu.SemaphoreType.DMA((8, 2, 2, nblk)),
                pltpu.SemaphoreType.DMA((2,)),
                pltpu.SemaphoreType.DMA((nblk,)),
            ],
            compiler_params=pltpu.CompilerParams(collective_id=0, has_side_effects=True, vmem_limit_bytes=46 * 1024 * 1024),
            name="layer",
        )(x_in, g_norm.reshape(width // LANES, LANES), jnp.asarray(rope_tables(tokens)), w_q, w_k, w_v, w_o, w_gate.T, w_up.T, w_down)
        y, k, v = pl.pallas_call(
            store_kernel,
            out_shape=(jax.ShapeDtypeStruct((tokens, width), BF16),
                       jax.ShapeDtypeStruct((tokens, HEAD_DIM), BF16),
                       jax.ShapeDtypeStruct((tokens, HEAD_DIM), BF16)),
            in_specs=[any_spec] * 3,
            out_specs=(any_spec,) * 3,
            scratch_shapes=[pltpu.SemaphoreType.DMA((10,))],
            compiler_params=pltpu.CompilerParams(vmem_limit_bytes=1024 * 1024),
            name="store",
        )(y, k, v)
        return y, k.reshape(tokens, 1, HEAD_DIM), v.reshape(tokens, 1, HEAD_DIM)

    return jax.shard_map(local_layer, mesh=mesh, in_specs=(P('dp', None), P(None), P(None, 'tp'), P(None, None), P(None, None), P('tp', None), P(None, 'tp'), P(None, 'tp'), P('tp', None)), out_specs=(P('dp', None), P('dp', 'tp', None), P('dp', 'tp', None)), check_vma=False)
```

```python
import functools
import math
import jax
import jax.numpy as jnp
import numpy as np
from jax import lax
from jax.experimental import pallas as pl
from jax.experimental.pallas import tpu as pltpu
from jax.sharding import PartitionSpec as P

HEAD_DIM = 128
ROPE_BASE = 500000.0
NORM_EPS = 1e-5
LANES = 128
ROWS = 128
SLOTS = 2
RING = 4
KEYS = 512
OUT_TILE = 512
LAG = (1, 2, 3, 4, 5, 6, 7, 8, 9, 10)
FIRST = (1, 2, 3)
SECOND = (4, 5, 6, 7, 8, 9, 10)
BF16 = jnp.bfloat16
F32 = jnp.float32


def layer_kernel(cfg, x_hbm, g_ref, tab_hbm, wq_hbm, wk_hbm, wv_hbm, wo_hbm, wg_hbm, wu_hbm, wd_hbm,
                 ybuf, kbuf, vbuf,
                 wall, wgu, wod, xbuf, tabs, abuf, gbuf, ombuf, part, quart, r1, r2, r3, r4, xres,
                 wsem, xsem, ressem, pair_send, pair_recv, ssem, rsem, gpair_send, gpair_recv):
    tokens, width = x_hbm.shape
    tp, side, kv_heads = cfg[:3]
    nblk = tokens // ROWS
    half = width // 2
    quarter = half // 2
    cw = quarter // side
    ch = cw // 2
    rw = ROWS // side
    ff = wg_hbm.shape[0]

    me = lax.axis_index("tp")
    core = lax.rem(me, 2)
    px = lax.rem(me // 2, side)
    py = me // (2 * side)
    partner = me + 1 - 2 * core

    def wrap(p):
        return lax.rem(p + side, side)

    def at(y, x):
        return (wrap(y) * side + wrap(x)) * 2 + core

    near = (((at(py, px + 1)), (at(py, px - 1))), ((at(py + 1, px)), (at(py - 1, px))))
    pos = (px, py)

    def dev(d):
        return {"tp": d}

    barrier = pltpu.get_barrier_semaphore()
    for d in (partner, *near[0], *near[1]):
        pl.semaphore_signal(barrier, inc=1, device_id=dev(d), device_id_type=pl.DeviceIdType.MESH)

    head = lax.div(me * kv_heads, tp)
    kcol = pl.ds(pl.multiple_of(head * HEAD_DIM, HEAD_DIM), HEAD_DIM)
    mine0 = core * half
    res_col = [pl.multiple_of(mine0 + ab * quarter + pos[ab] * cw, cw) for ab in (0, 1)]

    def x_load(b):
        rows = pl.ds(pl.multiple_of(b * ROWS, ROWS), ROWS)
        slot = lax.rem(b, 2)
        return (pltpu.make_async_copy(x_hbm.at[rows], xbuf, xsem.at[slot, 0]),
                pltpu.make_async_copy(tab_hbm.at[:, rows], tabs.at[slot], xsem.at[slot, 1]))

    w_loads = (
        pltpu.make_async_copy(wg_hbm, wgu.at[pl.ds(0, ff)], wsem.at[0]),
        pltpu.make_async_copy(wu_hbm, wgu.at[pl.ds(ff, ff)], wsem.at[1]),
        pltpu.make_async_copy(wq_hbm, wall.at[:, pl.ds(0, HEAD_DIM)], wsem.at[2]),
        pltpu.make_async_copy(wk_hbm.at[:, kcol], wall.at[:, pl.ds(HEAD_DIM, HEAD_DIM)], wsem.at[3]),
        pltpu.make_async_copy(wv_hbm.at[:, kcol], wall.at[:, pl.ds(2 * HEAD_DIM, HEAD_DIM)], wsem.at[4]),
        pltpu.make_async_copy(wo_hbm, wod.at[pl.ds(0, HEAD_DIM)], wsem.at[5]),
        pltpu.make_async_copy(wd_hbm, wod.at[pl.ds(HEAD_DIM, ff)], wsem.at[6]),
    )
    for c in x_load(0):
        c.start()
    for c in w_loads:
        c.start()
    res_loads = [pltpu.make_async_copy(x_hbm.at[:, pl.ds(res_col[ab], cw)], xres.at[ab], ressem.at[ab]) for ab in (0, 1)]
    for c in res_loads:
        c.start()
    kbuf[...] = jnp.zeros_like(kbuf)
    vbuf[...] = jnp.zeros_like(vbuf)

    def pair_copy(b):
        col = pl.multiple_of((1 - core) * half, half)
        return pltpu.make_async_remote_copy(
            src_ref=part.at[lax.rem(b, SLOTS), :, pl.ds(col, half)], dst_ref=quart.at[b],
            send_sem=pair_send.at[lax.rem(b, SLOTS)], recv_sem=pair_recv.at[b],
            device_id=dev(partner), device_id_type=pl.DeviceIdType.MESH)

    def hop(src, dst, st, b, ab, d, axis):
        return pltpu.make_async_remote_copy(
            src_ref=src, dst_ref=dst, send_sem=ssem.at[st, ab, d, lax.rem(b, 2)], recv_sem=rsem.at[st, ab, d, b],
            device_id=dev(near[axis][d]), device_id_type=pl.DeviceIdType.MESH)

    def qcols(ab, chunk, h=None):
        base = ab * quarter + wrap(chunk) * cw
        if h is None:
            return pl.ds(pl.multiple_of(base, cw), cw)
        return pl.ds(pl.multiple_of(base + h * ch, ch), ch)

    def ycols(ab, chunk, h=None):
        base = mine0 + ab * quarter + wrap(chunk) * cw
        if h is None:
            return pl.ds(pl.multiple_of(base, cw), cw)
        return pl.ds(pl.multiple_of(base + h * ch, ch), ch)

    def brows(chunk):
        return pl.ds(pl.multiple_of(wrap(chunk) * rw, rw), rw)

    def yrows(b, chunk=None):
        if chunk is None:
            return pl.ds(pl.multiple_of(b * ROWS, ROWS), ROWS)
        return pl.ds(pl.multiple_of(b * ROWS + wrap(chunk) * rw, rw), rw)

    def send1(b, ab, d):
        p = pos[ab]
        return hop(quart.at[b, :, qcols(ab, p + 2, d)], r1.at[lax.rem(b, RING), ab, d], 0, b, ab, d, ab)

    def send2(b, ab, d):
        p = pos[ab]
        return hop(quart.at[b, :, qcols(ab, p + 1 - 2 * d)], r2.at[lax.rem(b, RING), ab, d], 1, b, ab, d, ab)

    def send3(b, ab, d):
        p2 = pos[1 - ab]
        return hop(quart.at[b, brows(p2 + 2), qcols(ab, pos[ab], d)], r3.at[b, ab, d], 2, b, ab, d, 1 - ab)

    def send4(b, ab, d):
        p2 = pos[1 - ab]
        return hop(quart.at[b, brows(p2 + 1 - 2 * d), qcols(ab, pos[ab])], r4.at[b, ab, d], 3, b, ab, d, 1 - ab)

    def y_hop(b, rows, cols, st, ab, d, axis):
        return hop(ybuf.at[rows, cols], ybuf.at[rows, cols], st, b, ab, d, axis)

    def send5(b, ab, d):
        return y_hop(b, yrows(b, pos[1 - ab]), ycols(ab, pos[ab]), 4, ab, d, 1 - ab)

    def land5(b, ab, d):
        return y_hop(b, yrows(b, pos[1 - ab] - 1 + 2 * d), ycols(ab, pos[ab]), 4, ab, d, 1 - ab)

    def send6(b, ab, d):
        return y_hop(b, yrows(b, pos[1 - ab] - 1 + 2 * d), ycols(ab, pos[ab], d), 5, ab, d, 1 - ab)

    def land6(b, ab, d):
        return y_hop(b, yrows(b, pos[1 - ab] + 2), ycols(ab, pos[ab], d), 5, ab, d, 1 - ab)

    def send7(b, ab, d):
        return y_hop(b, yrows(b), ycols(ab, pos[ab]), 6, ab, d, ab)

    def land7(b, ab, d):
        return y_hop(b, yrows(b), ycols(ab, pos[ab] - 1 + 2 * d), 6, ab, d, ab)

    def send8(b, ab, d):
        return y_hop(b, yrows(b), ycols(ab, pos[ab] - 1 + 2 * d, d), 7, ab, d, ab)

    def land8(b, ab, d):
        return y_hop(b, yrows(b), ycols(ab, pos[ab] + 2, d), 7, ab, d, ab)

    sends = (send1, send2, send3, send4, send5, send6, send7, send8)

    def gpair(b, c):
        cols = pl.ds(pl.multiple_of(c * half, half), half)
        return pltpu.make_async_remote_copy(
            src_ref=ybuf.at[yrows(b), cols], dst_ref=ybuf.at[yrows(b), cols],
            send_sem=gpair_send.at[lax.rem(b, 2)], recv_sem=gpair_recv.at[b],
            device_id=dev(partner), device_id_type=pl.DeviceIdType.MESH)

    def wait_all(copies):
        for cp in copies:
            cp.wait()

    def issue(send, b):
        @pl.when(b >= 2)
        def _():
            both(lambda ab, d: send(b - 2, ab, d).wait_send())

        both(lambda ab, d: send(b, ab, d).start())

    def attend(q, b, keys):
        s = lax.dot_general(q, kbuf[pl.ds(0, keys), :], (((1,), (1,)), ((), ())), preferred_element_type=F32)
        edge = keys - KEYS
        tail = s[:, edge:]
        qpos = b * ROWS + lax.broadcasted_iota(jnp.int32, tail.shape, 0)
        kpos = edge + lax.broadcasted_iota(jnp.int32, tail.shape, 1)
        tail = jnp.where(kpos <= qpos, tail, -1e30)
        s = jnp.concatenate([s[:, :edge], tail], axis=1) if edge else tail
        top = jnp.max(s, axis=-1, keepdims=True)
        e = jnp.exp2((s - top) * (math.log2(math.e) / math.sqrt(HEAD_DIM)))
        probs = (e * (1.0 / jnp.sum(e, axis=-1, keepdims=True))).astype(BF16)
        o = jnp.dot(probs, vbuf[pl.ds(0, keys), :], preferred_element_type=F32)
        ombuf[:, pl.ds(0, HEAD_DIM)] = o.astype(BF16)

    def norm_rows(r):
        rows = pl.ds(r, 16)
        sums = [jnp.zeros((16, LANES), F32)] * 2
        for j in range(width // LANES):
            xr = xbuf[rows, pl.ds(j * LANES, LANES)].astype(F32)
            sums[j % 2] = sums[j % 2] + xr * xr
        mean = jnp.sum(sums[0] + sums[1], axis=-1, keepdims=True) * (1.0 / width)
        inv = jnp.broadcast_to(lax.rsqrt(mean + NORM_EPS), (16, LANES))
        for j in range(width // LANES):
            cols = pl.ds(j * LANES, LANES)
            abuf[rows, cols] = (xbuf[rows, cols].astype(F32) * inv * gbuf[:, cols]).astype(BF16)

    def prepare():
        for j in range(width // LANES):
            gbuf[:, j * LANES:(j + 1) * LANES] = jnp.broadcast_to(g_ref[j:j + 1, :].astype(F32), (16, LANES))
        wait_all(x_load(0))

        @pl.loop(0, ROWS // 16)
        def _(i):
            norm_rows(pl.multiple_of(i * 16, 16))

        for cp in x_load(1):
            cp.start()

        split = ff // LANES * LANES
        for first, last, load in ((0, split, 0), (split, 2 * ff, 1)):
            wait_all(w_loads[load:load + 1])

            @pl.loop(0, width // KEYS)
            def _(i, first=first, last=last):
                rows = pl.ds(pl.multiple_of(i * KEYS, KEYS), KEYS)
                for m in range(first, last, LANES):
                    wall[rows, pl.ds(3 * HEAD_DIM + m, LANES)] = wgu[pl.ds(m, LANES), rows].T

        wait_all(w_loads[2:5])

    tiles = width // OUT_TILE

    def compute(b):
        slot = lax.rem(b, 2)
        proj = jnp.dot(abuf[...], wall[...], preferred_element_type=F32)
        cos_t = tabs[slot, 0]
        sin_t = tabs[slot, 1]

        def rope(z):
            return (z * cos_t + pltpu.roll(z, HEAD_DIM // 2, 1) * sin_t).astype(BF16)

        q = rope(proj[:, :HEAD_DIM])
        rows = yrows(b)
        kbuf[rows, :] = rope(proj[:, HEAD_DIM:2 * HEAD_DIM])
        vbuf[rows, :] = proj[:, 2 * HEAD_DIM:3 * HEAD_DIM].astype(BF16)
        gate = proj[:, 3 * HEAD_DIM:3 * HEAD_DIM + ff]
        up = proj[:, 3 * HEAD_DIM + ff:]
        ombuf[:, pl.ds(HEAD_DIM, ff)] = (gate * jax.nn.sigmoid(gate) * up).astype(BF16)

        for n in range(tokens // KEYS):
            @pl.when(b * ROWS // KEYS == n)
            def _(n=n):
                attend(q, b, (n + 1) * KEYS)

    def finish(b):
        slot = lax.rem(b, 2)

        @pl.when(b == 0)
        def _():
            wait_all(w_loads[5:])

        @pl.when(b >= SLOTS)
        def _():
            pair_copy(b - SLOTS).wait_send()

        @pl.when(b + 1 < nblk)
        def _():
            wait_all(x_load(b + 1))

        om = ombuf[...]
        for n in range(tiles):
            cols = pl.ds(n * OUT_TILE, OUT_TILE)
            for r in range(n * ROWS // tiles, (n + 1) * ROWS // tiles, 16):
                norm_rows(r)
            part[slot, :, cols] = jnp.dot(om, wod[:, cols], preferred_element_type=F32).astype(BF16)
        pair_copy(b).start()

        @pl.when(b + 2 < nblk)
        def _():
            for cp in x_load(b + 2):
                cp.start()

    def add(dst, *srcs):
        if len(srcs) == 1:
            dst[...] = dst[...] + srcs[0][...]
            return
        total = dst[...].astype(F32)
        for s in srcs:
            total = total + s[...].astype(F32)
        dst[...] = total.astype(BF16)

    def both(f):
        for ab in (0, 1):
            for d in (0, 1):
                f(ab, d)

    def stage1(b):
        pair_copy(b).wait_recv()
        mine = pl.ds(pl.multiple_of(mine0, half), half)
        for r in range(0, ROWS, 32):
            add(quart.at[b, pl.ds(r, 32), :], part.at[lax.rem(b, SLOTS), pl.ds(r, 32), mine])
        issue(send1, b)

    def stage2(b):
        both(lambda ab, d: send1(b, ab, d).wait_recv())
        both(lambda ab, d: add(quart.at[b, :, qcols(ab, pos[ab] + 1 - 2 * d, d)], r1.at[lax.rem(b, RING), ab, d]))
        issue(send2, b)

    def stage3(b):
        both(lambda ab, d: send2(b, ab, d).wait_recv())
        for ab in (0, 1):
            add(quart.at[b, :, qcols(ab, pos[ab])], r2.at[lax.rem(b, RING), ab, 0], r2.at[lax.rem(b, RING), ab, 1])
        issue(send3, b)

    def stage4(b):
        both(lambda ab, d: send3(b, ab, d).wait_recv())
        both(lambda ab, d: add(quart.at[b, brows(pos[1 - ab] + 1 - 2 * d), qcols(ab, pos[ab], d)], r3.at[b, ab, d]))
        issue(send4, b)

    def stage5(b):
        @pl.when(b == 0)
        def _():
            for c in res_loads:
                c.wait()

        both(lambda ab, d: send4(b, ab, d).wait_recv())
        for ab in (0, 1):
            p2 = pos[1 - ab]
            total = quart[b, brows(p2), qcols(ab, pos[ab])].astype(F32)
            total = total + r4[b, ab, 0].astype(F32) + r4[b, ab, 1].astype(F32)
            total = total + xres[ab, yrows(b, p2), :].astype(F32)
            ybuf[yrows(b, p2), ycols(ab, pos[ab])] = total.astype(BF16)
        issue(send5, b)

    def stage6(b):
        both(lambda ab, d: land5(b, ab, d).wait_recv())
        issue(send6, b)

    def stage7(b):
        both(lambda ab, d: land6(b, ab, d).wait_recv())
        issue(send7, b)

    def stage8(b):
        both(lambda ab, d: land7(b, ab, d).wait_recv())
        issue(send8, b)

    def stage9(b):
        both(lambda ab, d: land8(b, ab, d).wait_recv())

        @pl.when(b >= 2)
        def _():
            gpair(b - 2, core).wait_send()

        gpair(b, core).start()

    def stage10(b):
        gpair(b, 1 - core).wait_recv()

    stages = (stage1, stage2, stage3, stage4, stage5, stage6, stage7, stage8, stage9, stage10)

    prepare()
    pl.semaphore_wait(barrier, 5)

    @pl.loop(0, nblk + LAG[-1])
    def _(t):
        def run(group):
            for n in group:
                b = t - LAG[n - 1]

                @pl.when((b >= 0) & (b < nblk))
                def _(b=b, n=n):
                    stages[n - 1](b)

        @pl.when(t < nblk)
        def _():
            compute(t)

        run(FIRST)

        @pl.when(t < nblk)
        def _():
            finish(t)

        run(SECOND)

    for b in range(nblk - SLOTS, nblk):
        pair_copy(b).wait_send()
    for b in range(nblk - 2, nblk):
        for send in sends:
            both(lambda ab, d: send(b, ab, d).wait_send())
        gpair(b, core).wait_send()


def store_kernel(y_ref, k_ref, v_ref, y_hbm, k_hbm, v_hbm, sems):
    pieces = sems.shape[0] - 2
    rows = y_ref.shape[0] // pieces
    copies = [pltpu.make_async_copy(y_ref.at[pl.ds(i * rows, rows)], y_hbm.at[pl.ds(i * rows, rows)], sems.at[i])
              for i in range(pieces)]
    copies.append(pltpu.make_async_copy(k_ref, k_hbm, sems.at[pieces]))
    copies.append(pltpu.make_async_copy(v_ref, v_hbm, sems.at[pieces + 1]))
    for cp in copies:
        cp.start()
    for cp in copies:
        cp.wait()


def rope_tables(tokens):
    inv_freq = np.float32(ROPE_BASE) ** (-np.arange(0, HEAD_DIM, 2, dtype=np.float32) / np.float32(HEAD_DIM))
    angles = np.arange(tokens, dtype=np.float32)[:, None] * inv_freq[None, :]
    cos_half, sin_half = np.cos(angles), np.sin(angles)
    return np.stack([np.concatenate([cos_half, cos_half], axis=1), np.concatenate([-sin_half, sin_half], axis=1)])


def solution(mesh):
    tp_size = mesh.shape['tp']
    side = math.isqrt(tp_size // 2)

    def local_layer(x_in, g_norm, w_q, w_k, w_v, w_o, w_gate, w_up, w_down):
        tokens, width = x_in.shape
        kv_heads = w_k.shape[1] // HEAD_DIM
        ff = w_gate.shape[1]
        nblk = tokens // ROWS
        half = width // 2
        cw = half // 2 // side
        rw = ROWS // side
        any_spec = pl.BlockSpec(memory_space=pl.ANY)
        y, k, v = pl.pallas_call(
            functools.partial(layer_kernel, (tp_size, side, kv_heads)),
            out_shape=(pltpu.VMEM((tokens, width), BF16),
                       pltpu.VMEM((tokens, HEAD_DIM), BF16),
                       pltpu.VMEM((tokens, HEAD_DIM), BF16)),
            in_specs=[any_spec, pl.BlockSpec(memory_space=pltpu.VMEM)] + [any_spec] * 8,
            out_specs=(pl.BlockSpec(memory_space=pltpu.VMEM),) * 3,
            scratch_shapes=[
                pltpu.VMEM((width, 3 * HEAD_DIM + 2 * ff), BF16),
                pltpu.VMEM((2 * ff, width), BF16),
                pltpu.VMEM((HEAD_DIM + ff, width), BF16),
                pltpu.VMEM((ROWS, width), BF16),
                pltpu.VMEM((2, 2, ROWS, HEAD_DIM), F32),
                pltpu.VMEM((ROWS, width), BF16),
                pltpu.VMEM((16, width), F32),
                pltpu.VMEM((ROWS, HEAD_DIM + ff), BF16),
                pltpu.VMEM((SLOTS, ROWS, width), BF16),
                pltpu.VMEM((nblk, ROWS, half), BF16),
                pltpu.VMEM((RING, 2, 2, ROWS, cw // 2), BF16),
                pltpu.VMEM((RING, 2, 2, ROWS, cw), BF16),
                pltpu.VMEM((nblk, 2, 2, rw, cw // 2), BF16),
                pltpu.VMEM((nblk, 2, 2, rw, cw), BF16),
                pltpu.VMEM((2, tokens, cw), BF16),
                pltpu.SemaphoreType.DMA((7,)),
                pltpu.SemaphoreType.DMA((2, 2)),
                pltpu.SemaphoreType.DMA((2,)),
                pltpu.SemaphoreType.DMA((SLOTS,)),
                pltpu.SemaphoreType.DMA((nblk,)),
                pltpu.SemaphoreType.DMA((8, 2, 2, 2)),
                pltpu.SemaphoreType.DMA((8, 2, 2, nblk)),
                pltpu.SemaphoreType.DMA((2,)),
                pltpu.SemaphoreType.DMA((nblk,)),
            ],
            compiler_params=pltpu.CompilerParams(collective_id=0, has_side_effects=True, vmem_limit_bytes=46 * 1024 * 1024),
            name="layer",
        )(x_in, g_norm.reshape(width // LANES, LANES), jnp.asarray(rope_tables(tokens)), w_q, w_k, w_v, w_o, w_gate.T, w_up.T, w_down)
        y, k, v = pl.pallas_call(
            store_kernel,
            out_shape=(jax.ShapeDtypeStruct((tokens, width), BF16),
                       jax.ShapeDtypeStruct((tokens, HEAD_DIM), BF16),
                       jax.ShapeDtypeStruct((tokens, HEAD_DIM), BF16)),
            in_specs=[any_spec] * 3,
            out_specs=(any_spec,) * 3,
            scratch_shapes=[pltpu.SemaphoreType.DMA((10,))],
            compiler_params=pltpu.CompilerParams(vmem_limit_bytes=1024 * 1024),
            name="store",
        )(y, k, v)
        return y, k.reshape(tokens, 1, HEAD_DIM), v.reshape(tokens, 1, HEAD_DIM)

    return jax.shard_map(local_layer, mesh=mesh, in_specs=(P('dp', None), P(None), P(None, 'tp'), P(None, None), P(None, None), P('tp', None), P(None, 'tp'), P(None, 'tp'), P('tp', None)), out_specs=(P('dp', None), P('dp', 'tp', None), P('dp', 'tp', None)), check_vma=False)
```
